32 devices in a mesh: dp: 8 (over z, x), mp: 4 (over y, core).
Axes of the slice: x: 2, y: 2, z: 4, core: 2. Of those that a mesh axis runs over, the one named last changes fastest.
Arguments:
- hidden: bfloat16 [16, 4608], P('dp'), may hold values from -6 to 6
- in_gain: float32 [1, 4608], replicated, may hold values from 0.5 to 1.5
- post_gain: float32 [1, 4608], replicated, may hold values from 0.5 to 1.5
- query_weight: bfloat16 [1, 4608, 2048], P(None, 'dp', 'mp'), may hold values from -0.09375 to 0.09375
- key_weight: bfloat16 [1, 4608, 1024], P(None, 'dp', 'mp'), may hold values from -0.09375 to 0.09375
- value_weight: bfloat16 [1, 4608, 1024], P(None, 'dp', 'mp'), may hold values from -0.09375 to 0.09375
- out_weight: bfloat16 [1, 2048, 4608], P(None, 'mp', 'dp'), may hold values from -0.125 to 0.125
- key_cache: bfloat16 [1, 16, 512, 8, 128], P(None, 'dp', 'mp'), may hold values from -6 to 6
- value_cache: bfloat16 [1, 16, 512, 8, 128], P(None, 'dp', 'mp'), may hold values from -6 to 6
- lengths: int32 [16], P('dp'), may hold values from 256 to 512
- windowed: int32 [1, 16], P(None, 'dp'), may hold values from 0 to 1
Outputs:
- hidden_out: bfloat16 [16, 4608], P('dp')
- new_keys: bfloat16 [1, 16, 8, 128], P(None, 'dp')
- new_values: bfloat16 [1, 16, 8, 128], P(None, 'dp')
The draws below stay inside these ranges and needn't reach their ends.
Inputs may be any that keep to these rules, and one draw needn't show every extreme that they name: `lengths`: every request has between 256 and 512 cached tokens. `windowed`: each flag is 0 or 1, for every layer and request.
All inputs are finite; a program needn't handle non-finite values.
Results may differ from the reference program's by a relative error of at most 0.008.
Values may be sent and summed in bfloat16 or wider, within the bound.
A program may use at most 64 MiB of HBM per device.

```python
import jax
import jax.numpy as jnp
from jax import lax

D = 4608
HEADS = 16
KV_HEADS = 8
HEAD_DIM = 128
LAYERS = 1
REQUESTS = 16
SEQ = 512
WINDOW = 256


def place_ends(entries, key, low, largest):
    spot = [jax.random.randint(jax.random.fold_in(key, axis), (), 0, length) for axis, length in enumerate(entries.shape)]
    main_axis = entries.shape.index(max(entries.shape))
    neighbour = spot[:main_axis] + [(spot[main_axis] + 1) % entries.shape[main_axis]] + spot[main_axis + 1:]
    return entries.at[tuple(spot)].set(low).at[tuple(neighbour)].set(largest)


def levels(rng, dims, split, low, largest):
    loudness = 1.0
    for axis_at, blocks in split:
        steps = jax.random.uniform(jax.random.fold_in(jax.random.fold_in(rng, 6), axis_at), (blocks,), jnp.float32, low / len(split), largest / len(split))
        loudness = loudness * jnp.repeat(jnp.exp(steps), dims[axis_at] // blocks).reshape((-1,) + (1,) * (len(dims) - 1 - axis_at))
    return loudness


def centred(own_key, shape, spread, bound, pieces=(), held_as=jnp.bfloat16):
    entries = spread * jax.random.normal(own_key, shape, jnp.float32)
    if pieces:
        entries = entries * levels(own_key, shape, pieces, -0.22, 0.18)
    return jnp.clip(entries, -bound, bound).astype(held_as)


def setup_inputs(seed: int = 0) -> dict:
    seeds = jax.random.split(jax.random.key(seed), 12)
    hidden = centred(seeds[0], (REQUESTS, D), 1.0, 6.0, ((0, 8),))
    in_gain = jnp.clip(1.0 + 0.1 * jax.random.normal(seeds[1], (LAYERS, D), jnp.float32), 0.5, 1.5)
    post_gain = jnp.clip(1.0 + 0.1 * jax.random.normal(seeds[2], (LAYERS, D), jnp.float32), 0.5, 1.5)
    query_weight = centred(seeds[3], (LAYERS, D, HEADS * HEAD_DIM), D ** -0.5, 0.09375, ((1, 8), (2, 4)))
    key_weight = centred(seeds[4], (LAYERS, D, KV_HEADS * HEAD_DIM), D ** -0.5, 0.09375, ((1, 8), (2, 4)))
    value_weight = centred(seeds[5], (LAYERS, D, KV_HEADS * HEAD_DIM), D ** -0.5, 0.09375, ((1, 8), (2, 4)))
    out_weight = centred(seeds[6], (LAYERS, HEADS * HEAD_DIM, D), (HEADS * HEAD_DIM) ** -0.5, 0.125, ((1, 4), (2, 8)))
    key_cache = centred(seeds[7], (LAYERS, REQUESTS, SEQ, KV_HEADS, HEAD_DIM), 1.0, 6.0, ((1, 8), (2, 4)))
    value_cache = centred(seeds[8], (LAYERS, REQUESTS, SEQ, KV_HEADS, HEAD_DIM), 1.0, 6.0, ((1, 8), (2, 4)))
    lengths = place_ends(jax.random.randint(seeds[9], (REQUESTS,), SEQ // 2, SEQ + 1), jax.random.fold_in(seeds[9], 1), SEQ // 2, SEQ).astype(jnp.int32)
    windowed = place_ends(jax.random.randint(seeds[10], (LAYERS, REQUESTS), 0, 2), jax.random.fold_in(seeds[10], 1), 0, 1).astype(jnp.int32)
    return dict(hidden=hidden, in_gain=in_gain, post_gain=post_gain, query_weight=query_weight, key_weight=key_weight, value_weight=value_weight, out_weight=out_weight, key_cache=key_cache, value_cache=value_cache, lengths=lengths, windowed=windowed)


EPSILON = 1e-06
SOFTCAP = 50.0
ROPE_BASE = 10000.0
NEGATIVE = -1e+30

def rms_scale(values, gain_row):
    values = values.astype(jnp.float32)
    mean_square = lax.optimization_barrier(jnp.mean(values * values, axis=-1, keepdims=True))
    return values * lax.rsqrt(mean_square + EPSILON) * gain_row.astype(jnp.float32)

def rotate(values, positions):
    half_dim = values.shape[-1] // 2
    frequency = jnp.power(ROPE_BASE, -2.0 * jnp.arange(half_dim, dtype=jnp.float32) / values.shape[-1])
    angles = positions.astype(jnp.float32)[:, None] * frequency[None, :]
    cosine = jnp.cos(angles)[:, None, :]
    sine_table = jnp.sin(angles)[:, None, :]
    front_half = values[..., :half_dim]
    back_half = values[..., half_dim:]
    return jnp.concatenate((front_half * cosine - back_half * sine_table, back_half * cosine + front_half * sine_table), axis=-1)

def attend_one(request_item):
    queries, keys, values, length, key_new, value_new, window_flag = request_item
    group_size = HEADS // KV_HEADS
    grouped = queries.astype(jnp.float32).reshape(KV_HEADS, group_size, HEAD_DIM)
    scores = jnp.einsum('kgd,skd->kgs', grouped, keys.astype(jnp.float32))
    scores = SOFTCAP * jnp.tanh(scores / SOFTCAP)
    positions = jnp.arange(SEQ, dtype=jnp.int32)
    usable = (positions < length) & ((window_flag == 0) | (positions > length - WINDOW))
    masked = jnp.where(usable, scores, NEGATIVE)
    self_score = jnp.einsum('kgd,kd->kg', grouped, key_new.astype(jnp.float32))
    self_score = SOFTCAP * jnp.tanh(self_score / SOFTCAP)
    peak = jnp.maximum(lax.optimization_barrier(jnp.max(masked, axis=-1)), self_score)
    exp_scores = jnp.where(usable, jnp.exp(masked - peak[..., None]), 0.0)
    self_weight = jnp.exp(self_score - peak)
    denominator = lax.optimization_barrier(jnp.sum(exp_scores, axis=-1)) + self_weight
    mixed = jnp.einsum('kgs,skd->kgd', exp_scores, values.astype(jnp.float32))
    mixed = mixed + self_weight[..., None] * value_new.astype(jnp.float32)[:, None, :]
    return (mixed / denominator[..., None]).reshape(HEADS * HEAD_DIM)

def reference(hidden, in_gain, post_gain, query_weight, key_weight, value_weight, out_weight, key_cache, value_cache, lengths, windowed):
    keys_out = []
    values_out = []
    for layer_index in range(LAYERS):
        normed = rms_scale(hidden, in_gain[layer_index]).astype(jnp.bfloat16)
        query = jnp.dot(normed, query_weight[layer_index], preferred_element_type=jnp.float32).astype(jnp.bfloat16)
        key_raw = jnp.dot(normed, key_weight[layer_index], preferred_element_type=jnp.float32).astype(jnp.bfloat16)
        value_new = jnp.dot(normed, value_weight[layer_index], preferred_element_type=jnp.float32).astype(jnp.bfloat16)
        query = lax.optimization_barrier(query)
        key_raw = lax.optimization_barrier(key_raw)
        queries = rotate(query.astype(jnp.float32).reshape(-1, HEADS, HEAD_DIM), lengths)
        queries = (queries * HEAD_DIM ** (-0.5)).astype(jnp.bfloat16)
        keys_new = rotate(key_raw.astype(jnp.float32).reshape(-1, KV_HEADS, HEAD_DIM), lengths).astype(jnp.bfloat16)
        value_new = value_new.reshape(-1, KV_HEADS, HEAD_DIM)
        attended = lax.map(attend_one, (queries, key_cache[layer_index], value_cache[layer_index], lengths, keys_new, value_new, windowed[layer_index]))
        attended = attended.astype(jnp.bfloat16)
        projected = jnp.dot(attended, out_weight[layer_index], preferred_element_type=jnp.float32)
        hidden = (hidden.astype(jnp.float32) + rms_scale(projected, post_gain[layer_index])).astype(jnp.bfloat16)
        keys_out.append(keys_new)
        values_out.append(value_new)
    return (hidden, jnp.stack(keys_out), jnp.stack(values_out))
```

```python
import functools
import math

import jax
import jax.numpy as jnp
from jax import lax
from jax.experimental import pallas as pl
from jax.experimental.pallas import tpu as pltpu
from jax.sharding import PartitionSpec as P

HEADS = 16
KV_HEADS = 8
HEAD_DIM = 128
LAYERS = 1


EPSILON = 1e-06
SOFTCAP = 50.0
ROPE_BASE = 10000.0
NEGATIVE = -1e30


def rms_scale(values, gain_row):
    values = values.astype(jnp.float32)
    mean_square = jnp.mean(values * values, axis=-1, keepdims=True)
    return values * lax.rsqrt(mean_square + EPSILON) * gain_row.astype(jnp.float32)


def rotate(values, positions):
    half_dim = values.shape[-1] // 2
    frequency = jnp.power(
        ROPE_BASE, -2.0 * jnp.arange(half_dim, dtype=jnp.float32) / values.shape[-1]
    )
    angles = positions.astype(jnp.float32)[:, None] * frequency[None, :]
    cosine = jnp.cos(angles)[:, None, :]
    sine_table = jnp.sin(angles)[:, None, :]
    front_half = values[..., :half_dim]
    back_half = values[..., half_dim:]
    return jnp.concatenate(
        (
            front_half * cosine - back_half * sine_table,
            back_half * cosine + front_half * sine_table,
        ),
        axis=-1,
    )


def on_device(
    hidden,
    in_gain,
    post_gain,
    query_weight,
    key_weight,
    value_weight,
    out_weight,
    key_cache,
    value_cache,
    lengths,
    windowed,
):
    row_count = hidden.shape[0]
    query_width = query_weight.shape[2]
    key_width = key_weight.shape[2]
    seq_block = key_cache.shape[2]
    head_width = out_weight.shape[1]
    group_size = HEADS // KV_HEADS
    window_len = seq_block * lax.axis_size("mp") // 2
    keys_out = []
    values_out = []
    for layer_index in range(LAYERS):
        normed = rms_scale(hidden, in_gain[layer_index]).astype(jnp.bfloat16)
        token_slab = lax.all_to_all(normed, "dp", split_axis=1, concat_axis=0, tiled=True)
        joined = jnp.concatenate(
            (query_weight[layer_index], key_weight[layer_index], value_weight[layer_index]), 1
        )

        def local_term():
            part_rows = lax.slice_in_dim(token_slab, 0, row_count * lax.axis_size("dp"), axis=0)
            return jnp.dot(part_rows, joined, preferred_element_type=jnp.float32)

        summed = lax.psum_scatter(local_term(), "dp", scatter_dimension=0, tiled=True)
        query_part = summed[:, :query_width]
        key_part = summed[:, query_width : query_width + key_width]
        value_part = summed[:, query_width + key_width :]
        rounded = (
            query_part.astype(jnp.bfloat16),
            key_part.astype(jnp.bfloat16),
            value_part.astype(jnp.bfloat16),
        )
        query, key_raw, value_new = (
            lax.all_gather(rounded[0], "mp", axis=1, tiled=True),
            lax.all_gather(rounded[1], "mp", axis=1, tiled=True),
            lax.all_gather(rounded[2], "mp", axis=1, tiled=True),
        )
        queries = rotate(query.astype(jnp.float32).reshape(row_count, HEADS, HEAD_DIM), lengths)
        queries = (queries * HEAD_DIM ** (-0.5)).astype(jnp.bfloat16)
        keys_new = rotate(
            key_raw.astype(jnp.float32).reshape(row_count, KV_HEADS, HEAD_DIM), lengths
        ).astype(jnp.bfloat16)
        value_new = value_new.reshape(row_count, KV_HEADS, HEAD_DIM)
        grouped = queries.reshape(row_count, KV_HEADS, group_size, HEAD_DIM)
        scores = jnp.einsum(
            "rkgd,rskd->rkgs", grouped, key_cache[layer_index], preferred_element_type=jnp.float32
        )
        scores = SOFTCAP * jnp.tanh(scores / SOFTCAP)
        positions = lax.axis_index("mp") * seq_block + jnp.arange(seq_block, dtype=jnp.int32)
        window_flag = windowed[layer_index][:, None]
        usable = (positions[None, :] < lengths[:, None]) & (
            (window_flag == 0) | (positions[None, :] > lengths[:, None] - window_len)
        )
        usable = usable[:, None, None, :]
        masked = jnp.where(usable, scores, NEGATIVE)
        peaks = jnp.max(masked, axis=-1)
        exp_scores = jnp.where(usable, jnp.exp(masked - peaks[..., None]), 0.0)
        sums_exp = jnp.sum(exp_scores, axis=-1)
        accumulated = jnp.einsum(
            "rkgs,rskd->rkgd",
            exp_scores,
            value_cache[layer_index].astype(jnp.float32),
            preferred_element_type=jnp.float32,
        )
        global_peak = lax.pmax(peaks, "mp")
        rescale = jnp.exp(peaks - global_peak)
        sums_exp, accumulated = lax.psum(
            (sums_exp * rescale, accumulated * rescale[..., None]), "mp"
        )
        peaks = global_peak
        self_score = jnp.einsum(
            "rkgd,rkd->rkg", grouped, keys_new, preferred_element_type=jnp.float32
        )
        self_score = SOFTCAP * jnp.tanh(self_score / SOFTCAP)
        peak_all = jnp.maximum(peaks, self_score)
        old_scale = jnp.exp(peaks - peak_all)
        self_weight = jnp.exp(self_score - peak_all)
        denominator = sums_exp * old_scale + self_weight
        mixed = (
            accumulated * old_scale[..., None]
            + self_weight[..., None] * value_new.astype(jnp.float32)[:, :, None, :]
        )
        attended = (
            (mixed / denominator[..., None])
            .reshape(row_count, HEADS * HEAD_DIM)
            .astype(jnp.bfloat16)
        )
        attended_local = lax.dynamic_slice_in_dim(
            attended, lax.axis_index("mp") * head_width, head_width, 1
        )
        all_rows = lax.all_gather(attended_local, "dp", axis=0, tiled=True)
        partial_cols = jnp.dot(
            all_rows, out_weight[layer_index], preferred_element_type=jnp.float32
        )
        partial_cols = lax.psum(partial_cols, "mp")
        projected = lax.all_to_all(partial_cols, "dp", split_axis=0, concat_axis=1, tiled=True)
        hidden = (hidden.astype(jnp.float32) + rms_scale(projected, post_gain[layer_index])).astype(
            jnp.bfloat16
        )
        keys_out.append(keys_new)
        values_out.append(value_new)
    return (hidden, jnp.stack(keys_out), jnp.stack(values_out))


MESH_ID = pl.DeviceIdType.MESH
BLOCK_ROWS = 8


def fits(mesh):
    parts = mesh.shape["mp"]
    query_heads = HEADS // parts
    key_heads = KV_HEADS // parts
    return (
        HEADS % parts == 0
        and KV_HEADS % parts == 0
        and query_heads == 2 * key_heads
        and query_heads + 2 * key_heads == BLOCK_ROWS
    )


def one_hot(rows, columns, match):
    row = lax.broadcasted_iota(jnp.int32, (rows, columns), 0)
    column = lax.broadcasted_iota(jnp.int32, (rows, columns), 1)
    return jnp.where(match(row, column), 1.0, 0.0).astype(jnp.bfloat16)


def pick(selector, values):
    return jnp.dot(selector, values, preferred_element_type=jnp.float32)


def fused_kernel(
    dp,
    mp,
    lengths_ref,
    windowed_ref,
    hidden_ref,
    in_gain_ref,
    post_gain_ref,
    query_hbm,
    key_hbm,
    value_hbm,
    out_hbm,
    key_cache_hbm,
    value_cache_hbm,
    hidden_out_ref,
    new_keys_ref,
    new_values_ref,
    query_w,
    key_w,
    value_w,
    out_w,
    keys,
    values,
    norm_send,
    norm_recv,
    proj_send,
    proj_recv,
    mix_send,
    mix_recv,
    cols_send,
    cols_recv,
    load_sem,
    send_sem,
    recv_sem,
):
    my_dp = lax.axis_index("dp")
    my_mp = lax.axis_index("mp")
    devices = dp * mp
    me = my_dp * mp + my_mp
    rows = hidden_ref.shape[0]
    total_rows = rows * dp
    slab = norm_send.shape[2]
    query_width = query_w.shape[1]
    key_width = key_w.shape[1]
    query_heads = query_width // HEAD_DIM
    key_heads = key_width // HEAD_DIM
    seq_block = key_cache_hbm.shape[2]
    cache_rows = seq_block * KV_HEADS
    window_len = seq_block * mp // 2

    loads = [
        pltpu.make_async_copy(src, dst, load_sem.at[i])
        for i, (src, dst) in enumerate(
            (
                (query_hbm.at[0], query_w),
                (key_hbm.at[0], key_w),
                (value_hbm.at[0], value_w),
                (key_cache_hbm.at[0], keys),
                (value_cache_hbm.at[0], values),
                (out_hbm.at[0], out_w),
            )
        )
    ]
    barrier = pltpu.get_barrier_semaphore()
    for step in range(1, devices):
        there = lax.rem(me + step, devices)
        pl.semaphore_signal(
            barrier,
            inc=1,
            device_id={"dp": there // mp, "mp": lax.rem(there, mp)},
            device_id_type=MESH_ID,
        )
    for load in loads:
        load.start()

    hidden = hidden_ref[...].astype(jnp.float32)
    mean_square = jnp.mean(hidden * hidden, axis=-1, keepdims=True)
    normed = hidden * lax.rsqrt(mean_square + EPSILON) * in_gain_ref[...]
    for part in range(dp):
        norm_send[part] = normed[:, part * slab : (part + 1) * slab].astype(jnp.bfloat16)
    norm_recv[my_dp] = norm_send[my_dp]

    pl.semaphore_wait(barrier, devices - 1)
    for step in range(1, dp):
        there = lax.rem(my_dp + step, dp)
        pltpu.make_async_remote_copy(
            src_ref=norm_send.at[there],
            dst_ref=norm_recv.at[my_dp],
            send_sem=send_sem.at[0],
            recv_sem=recv_sem.at[0],
            device_id={"dp": there, "mp": my_mp},
            device_id_type=MESH_ID,
        ).start()

    def finish(buffer, count, sem):
        block = buffer.at[pl.ds(0, count)]
        pltpu.make_async_copy(block, block, sem).wait()

    def scatter(send, recv, stage, slot_of):
        for step in range(1, devices):
            there = lax.rem(me + step, devices)
            there_dp = there // mp
            there_mp = lax.rem(there, mp)
            pltpu.make_async_remote_copy(
                src_ref=send.at[slot_of(there_dp, there_mp)],
                dst_ref=recv.at[me],
                send_sem=send_sem.at[stage],
                recv_sem=recv_sem.at[stage],
                device_id={"dp": there_dp, "mp": there_mp},
                device_id_type=MESH_ID,
            ).start()
        recv[me] = send[slot_of(my_dp, my_mp)]

    lane = lax.broadcasted_iota(jnp.int32, (BLOCK_ROWS, HEAD_DIM), 1)
    half = HEAD_DIM // 2
    pair = jnp.where(lane < half, lane, lane - half).astype(jnp.float32)
    frequency = jnp.exp(pair * (-2.0 / HEAD_DIM * math.log(ROPE_BASE)))
    cosines = []
    sines = []
    for r in range(rows):
        angle = lengths_ref[r].astype(jnp.float32) * frequency
        cosines.append(jnp.cos(angle))
        sine = jnp.sin(angle)
        sines.append(jnp.where(lane < half, -sine, sine))

    for load in loads[:3]:
        load.wait()
    finish(norm_recv, dp - 1, recv_sem.at[0])
    tokens = jnp.concatenate(
        [norm_recv[part].astype(jnp.float32) for part in range(dp)], axis=0
    ).astype(jnp.bfloat16)
    parts = [
        jnp.dot(tokens, weight[...], preferred_element_type=jnp.float32)
        for weight in (query_w, key_w, value_w)
    ]
    pieces = []
    for part in parts:
        for at in range(0, part.shape[1], HEAD_DIM):
            pieces.append(part[:, at : at + HEAD_DIM])
    stacked = jnp.concatenate(pieces, axis=0).astype(jnp.bfloat16)
    spread = one_hot(
        total_rows * BLOCK_ROWS,
        total_rows * BLOCK_ROWS,
        lambda row, column: column
        == (row % BLOCK_ROWS) * total_rows + row // BLOCK_ROWS,
    )
    proj_send[...] = (
        pick(spread, stacked).astype(jnp.bfloat16).reshape(dp, rows * BLOCK_ROWS, HEAD_DIM)
    )
    scatter(proj_send, proj_recv, 1, lambda there_dp, there_mp: there_dp)

    for load in loads[3:5]:
        load.wait()
    group_rows = mp * BLOCK_ROWS
    row = lax.broadcasted_iota(jnp.int32, (group_rows, cache_rows), 0)
    column = lax.broadcasted_iota(jnp.int32, (group_rows, cache_rows), 1)
    in_block = row % BLOCK_ROWS
    head_match = (in_block < query_heads) & (
        column % KV_HEADS == (row // BLOCK_ROWS) * key_heads + in_block // 2
    )
    position = my_mp * seq_block + column // KV_HEADS
    allowed = []
    for r in range(rows):
        length = lengths_ref[r]
        floor = jnp.where(windowed_ref[0, r] == 0, -1, length - window_len)
        allowed.append(head_match & (position < length) & (position > floor))
    self_row = lax.broadcasted_iota(jnp.int32, (group_rows, group_rows), 0)
    self_column = lax.broadcasted_iota(jnp.int32, (group_rows, group_rows), 1)
    self_slot = self_row % BLOCK_ROWS
    own_base = (self_row // BLOCK_ROWS) * BLOCK_ROWS + query_heads + self_slot // 2
    is_query = self_slot < query_heads
    self_key = is_query & (self_column == own_base)
    self_value = jnp.where(is_query & (self_column == own_base + key_heads), 1.0, 0.0).astype(
        jnp.bfloat16
    )
    acc_row = lax.broadcasted_iota(jnp.int32, (group_rows, HEAD_DIM), 0) % BLOCK_ROWS
    self_share = jnp.where(my_mp == 0, 1.0, 0.0)

    finish(proj_recv, devices - 1, recv_sem.at[1])
    blocks = rows * BLOCK_ROWS
    summed = jnp.sum(
        proj_recv[...].astype(jnp.float32).reshape(dp, mp, blocks, HEAD_DIM), axis=0
    )
    rotated_rows = []
    raw_rows = []
    for r in range(rows):
        raw = summed[:, r * BLOCK_ROWS : (r + 1) * BLOCK_ROWS, :].reshape(group_rows, HEAD_DIM)
        raw = raw.astype(jnp.bfloat16)
        wide = raw.astype(jnp.float32)
        cosine = jnp.concatenate([cosines[r]] * mp, axis=0)
        sine = jnp.concatenate([sines[r]] * mp, axis=0)
        turned = wide * cosine + pltpu.roll(wide, half, 1) * sine
        queries = (turned * HEAD_DIM ** (-0.5)).astype(jnp.bfloat16)
        turned = turned.astype(jnp.bfloat16)
        rotated_rows.append(turned)
        raw_rows.append(raw)
        flat_keys = keys[r].reshape(cache_rows, HEAD_DIM)
        flat_values = values[r].reshape(cache_rows, HEAD_DIM)
        over_last = (((1,), (1,)), ((), ()))
        scores = lax.dot_general(
            queries, flat_keys, over_last, preferred_element_type=jnp.float32
        )
        scores = SOFTCAP * jnp.tanh(scores / SOFTCAP)
        exp_scores = jnp.where(allowed[r], jnp.exp(scores), 0.0)
        sums_exp = jnp.sum(exp_scores, axis=-1, keepdims=True)
        accumulated = jnp.dot(
            exp_scores.astype(jnp.bfloat16), flat_values, preferred_element_type=jnp.float32
        )
        own = lax.dot_general(queries, turned, over_last, preferred_element_type=jnp.float32)
        own = jnp.sum(jnp.where(self_key, own, 0.0), axis=-1, keepdims=True)
        own = jnp.exp(SOFTCAP * jnp.tanh(own / SOFTCAP)) * self_share
        accumulated = accumulated + own * pick(self_value, raw)
        sums_exp = jnp.broadcast_to(sums_exp + own, (group_rows, HEAD_DIM))
        message = jnp.where(
            acc_row < query_heads, accumulated, pltpu.roll(sums_exp, query_heads, 0)
        )
        mix_send[:, r * BLOCK_ROWS : (r + 1) * BLOCK_ROWS, :] = message.reshape(
            mp, BLOCK_ROWS, HEAD_DIM
        ).astype(mix_send.dtype)
    scatter(mix_send, mix_recv, 2, lambda there_dp, there_mp: there_mp)

    turned_all = jnp.concatenate(rotated_rows, axis=0)
    raw_all = jnp.concatenate(raw_rows, axis=0)

    def owner(row, first):
        head = row % KV_HEADS
        return (
            (row // KV_HEADS) * group_rows
            + (head // key_heads) * BLOCK_ROWS
            + first
            + head % key_heads
        )

    key_rows = one_hot(
        rows * KV_HEADS, rows * group_rows, lambda row, column: column == owner(row, query_heads)
    )
    value_rows = one_hot(
        rows * KV_HEADS,
        rows * group_rows,
        lambda row, column: column == owner(row, query_heads + key_heads),
    )
    new_keys_ref[...] = (
        pick(key_rows, turned_all).astype(jnp.bfloat16).reshape(new_keys_ref.shape)
    )
    new_values_ref[...] = (
        pick(value_rows, raw_all).astype(jnp.bfloat16).reshape(new_values_ref.shape)
    )
    gather = one_hot(
        query_heads * total_rows,
        total_rows * BLOCK_ROWS,
        lambda row, column: column
        == (row % total_rows) * BLOCK_ROWS + row // total_rows,
    )

    loads[5].wait()
    finish(mix_recv, devices - 1, recv_sem.at[2])
    mixed = jnp.sum(
        mix_recv[...].astype(jnp.float32).reshape(dp, mp, blocks, HEAD_DIM), axis=1
    ).reshape(dp * blocks, HEAD_DIM)
    all_row = lax.broadcasted_iota(jnp.int32, mixed.shape, 0) % BLOCK_ROWS
    weights = pltpu.roll(mixed, mixed.shape[0] - query_heads, 0)
    attended = jnp.where(all_row < query_heads, mixed / weights, 0.0).astype(jnp.bfloat16)
    heads = pick(gather, attended).astype(jnp.bfloat16)
    heads = jnp.concatenate(
        [heads[b * total_rows : (b + 1) * total_rows] for b in range(query_heads)], axis=1
    )
    partial_cols = jnp.dot(heads, out_w[...], preferred_element_type=jnp.float32)
    for part in range(dp):
        cols_send[part] = partial_cols[part * rows : (part + 1) * rows].astype(cols_send.dtype)
    scatter(cols_send, cols_recv, 3, lambda there_dp, there_mp: there_dp)
    finish(cols_recv, devices - 1, recv_sem.at[3])
    pieces = []
    for part in range(dp):
        piece = cols_recv[part * mp].astype(jnp.float32)
        for other in range(1, mp):
            piece = piece + cols_recv[part * mp + other].astype(jnp.float32)
        pieces.append(piece)
    projected = jnp.concatenate(pieces, axis=1)
    mean_square = jnp.mean(projected * projected, axis=-1, keepdims=True)
    update = projected * lax.rsqrt(mean_square + EPSILON) * post_gain_ref[...]
    hidden_out_ref[...] = (hidden_ref[...].astype(jnp.float32) + update).astype(jnp.bfloat16)

    finish(norm_recv, dp - 1, send_sem.at[0])
    finish(proj_recv, devices - 1, send_sem.at[1])
    finish(mix_recv, devices - 1, send_sem.at[2])
    finish(cols_recv, devices - 1, send_sem.at[3])


def fused_device(
    hidden,
    in_gain,
    post_gain,
    query_weight,
    key_weight,
    value_weight,
    out_weight,
    key_cache,
    value_cache,
    lengths,
    windowed,
):
    dp = lax.axis_size("dp")
    mp = lax.axis_size("mp")
    rows = hidden.shape[0]
    slab = query_weight.shape[1]
    out_slab = out_weight.shape[2]
    blocks = rows * BLOCK_ROWS
    half_word = jnp.bfloat16
    smem = pl.BlockSpec(memory_space=pltpu.SMEM)
    vmem = pl.BlockSpec(memory_space=pltpu.VMEM)
    far = pl.BlockSpec(memory_space=pl.ANY)
    return pl.pallas_call(
        functools.partial(fused_kernel, dp, mp),
        out_shape=(
            jax.ShapeDtypeStruct(hidden.shape, half_word),
            jax.ShapeDtypeStruct((LAYERS, rows, KV_HEADS, HEAD_DIM), half_word),
            jax.ShapeDtypeStruct((LAYERS, rows, KV_HEADS, HEAD_DIM), half_word),
        ),
        in_specs=[smem, smem, vmem, vmem, vmem, far, far, far, far, far, far],
        out_specs=(vmem, vmem, vmem),
        scratch_shapes=[
            pltpu.VMEM(query_weight.shape[1:], half_word),
            pltpu.VMEM(key_weight.shape[1:], half_word),
            pltpu.VMEM(value_weight.shape[1:], half_word),
            pltpu.VMEM(out_weight.shape[1:], half_word),
            pltpu.VMEM(key_cache.shape[1:], half_word),
            pltpu.VMEM(value_cache.shape[1:], half_word),
            pltpu.VMEM((dp, rows, slab), half_word),
            pltpu.VMEM((dp, rows, slab), half_word),
            pltpu.VMEM((dp, blocks, HEAD_DIM), half_word),
            pltpu.VMEM((dp * mp, blocks, HEAD_DIM), half_word),
            pltpu.VMEM((mp, blocks, HEAD_DIM), half_word),
            pltpu.VMEM((dp * mp, blocks, HEAD_DIM), half_word),
            pltpu.VMEM((dp, rows, out_slab), half_word),
            pltpu.VMEM((dp * mp, rows, out_slab), half_word),
            pltpu.SemaphoreType.DMA((6,)),
            pltpu.SemaphoreType.DMA((4,)),
            pltpu.SemaphoreType.DMA((4,)),
        ],
        compiler_params=pltpu.CompilerParams(collective_id=0, has_side_effects=True),
    )(
        lengths,
        windowed,
        hidden,
        in_gain,
        post_gain,
        query_weight,
        key_weight,
        value_weight,
        out_weight,
        key_cache,
        value_cache,
    )


def solution(mesh):
    return jax.shard_map(
        fused_device if fits(mesh) else on_device,
        mesh=mesh,
        in_specs=(
            P("dp", None),
            P(),
            P(),
            P(None, "dp", "mp"),
            P(None, "dp", "mp"),
            P(None, "dp", "mp"),
            P(None, "mp", "dp"),
            P(None, "dp", "mp", None, None),
            P(None, "dp", "mp", None, None),
            P("dp"),
            P(None, "dp"),
        ),
        out_specs=(P("dp", None), P(None, "dp", None, None), P(None, "dp", None, None)),
        check_vma=False,
    )
```

```python
import functools
import math

import jax
import jax.numpy as jnp
from jax import lax
from jax.experimental import pallas as pl
from jax.experimental.pallas import tpu as pltpu
from jax.sharding import PartitionSpec as P

HEADS = 16
KV_HEADS = 8
HEAD_DIM = 128
LAYERS = 1


EPSILON = 1e-06
SOFTCAP = 50.0
ROPE_BASE = 10000.0
NEGATIVE = -1e30


def rms_scale(values, gain_row):
    values = values.astype(jnp.float32)
    mean_square = jnp.mean(values * values, axis=-1, keepdims=True)
    return values * lax.rsqrt(mean_square + EPSILON) * gain_row.astype(jnp.float32)


def rotate(values, positions):
    half_dim = values.shape[-1] // 2
    frequency = jnp.power(
        ROPE_BASE, -2.0 * jnp.arange(half_dim, dtype=jnp.float32) / values.shape[-1]
    )
    angles = positions.astype(jnp.float32)[:, None] * frequency[None, :]
    cosine = jnp.cos(angles)[:, None, :]
    sine_table = jnp.sin(angles)[:, None, :]
    front_half = values[..., :half_dim]
    back_half = values[..., half_dim:]
    return jnp.concatenate(
        (
            front_half * cosine - back_half * sine_table,
            back_half * cosine + front_half * sine_table,
        ),
        axis=-1,
    )


def on_device(
    hidden,
    in_gain,
    post_gain,
    query_weight,
    key_weight,
    value_weight,
    out_weight,
    key_cache,
    value_cache,
    lengths,
    windowed,
):
    row_count = hidden.shape[0]
    query_width = query_weight.shape[2]
    key_width = key_weight.shape[2]
    seq_block = key_cache.shape[2]
    head_width = out_weight.shape[1]
    group_size = HEADS // KV_HEADS
    window_len = seq_block * lax.axis_size("mp") // 2
    keys_out = []
    values_out = []
    for layer_index in range(LAYERS):
        normed = rms_scale(hidden, in_gain[layer_index]).astype(jnp.bfloat16)
        token_slab = lax.all_to_all(normed, "dp", split_axis=1, concat_axis=0, tiled=True)
        joined = jnp.concatenate(
            (query_weight[layer_index], key_weight[layer_index], value_weight[layer_index]), 1
        )

        def local_term():
            part_rows = lax.slice_in_dim(token_slab, 0, row_count * lax.axis_size("dp"), axis=0)
            return jnp.dot(part_rows, joined, preferred_element_type=jnp.float32)

        summed = lax.psum_scatter(local_term(), "dp", scatter_dimension=0, tiled=True)
        query_part = summed[:, :query_width]
        key_part = summed[:, query_width : query_width + key_width]
        value_part = summed[:, query_width + key_width :]
        rounded = (
            query_part.astype(jnp.bfloat16),
            key_part.astype(jnp.bfloat16),
            value_part.astype(jnp.bfloat16),
        )
        query, key_raw, value_new = (
            lax.all_gather(rounded[0], "mp", axis=1, tiled=True),
            lax.all_gather(rounded[1], "mp", axis=1, tiled=True),
            lax.all_gather(rounded[2], "mp", axis=1, tiled=True),
        )
        queries = rotate(query.astype(jnp.float32).reshape(row_count, HEADS, HEAD_DIM), lengths)
        queries = (queries * HEAD_DIM ** (-0.5)).astype(jnp.bfloat16)
        keys_new = rotate(
            key_raw.astype(jnp.float32).reshape(row_count, KV_HEADS, HEAD_DIM), lengths
        ).astype(jnp.bfloat16)
        value_new = value_new.reshape(row_count, KV_HEADS, HEAD_DIM)
        grouped = queries.reshape(row_count, KV_HEADS, group_size, HEAD_DIM)
        scores = jnp.einsum(
            "rkgd,rskd->rkgs", grouped, key_cache[layer_index], preferred_element_type=jnp.float32
        )
        scores = SOFTCAP * jnp.tanh(scores / SOFTCAP)
        positions = lax.axis_index("mp") * seq_block + jnp.arange(seq_block, dtype=jnp.int32)
        window_flag = windowed[layer_index][:, None]
        usable = (positions[None, :] < lengths[:, None]) & (
            (window_flag == 0) | (positions[None, :] > lengths[:, None] - window_len)
        )
        usable = usable[:, None, None, :]
        masked = jnp.where(usable, scores, NEGATIVE)
        peaks = jnp.max(masked, axis=-1)
        exp_scores = jnp.where(usable, jnp.exp(masked - peaks[..., None]), 0.0)
        sums_exp = jnp.sum(exp_scores, axis=-1)
        accumulated = jnp.einsum(
            "rkgs,rskd->rkgd",
            exp_scores,
            value_cache[layer_index].astype(jnp.float32),
            preferred_element_type=jnp.float32,
        )
        global_peak = lax.pmax(peaks, "mp")
        rescale = jnp.exp(peaks - global_peak)
        sums_exp, accumulated = lax.psum(
            (sums_exp * rescale, accumulated * rescale[..., None]), "mp"
        )
        peaks = global_peak
        self_score = jnp.einsum(
            "rkgd,rkd->rkg", grouped, keys_new, preferred_element_type=jnp.float32
        )
        self_score = SOFTCAP * jnp.tanh(self_score / SOFTCAP)
        peak_all = jnp.maximum(peaks, self_score)
        old_scale = jnp.exp(peaks - peak_all)
        self_weight = jnp.exp(self_score - peak_all)
        denominator = sums_exp * old_scale + self_weight
        mixed = (
            accumulated * old_scale[..., None]
            + self_weight[..., None] * value_new.astype(jnp.float32)[:, :, None, :]
        )
        attended = (
            (mixed / denominator[..., None])
            .reshape(row_count, HEADS * HEAD_DIM)
            .astype(jnp.bfloat16)
        )
        attended_local = lax.dynamic_slice_in_dim(
            attended, lax.axis_index("mp") * head_width, head_width, 1
        )
        all_rows = lax.all_gather(attended_local, "dp", axis=0, tiled=True)
        partial_cols = jnp.dot(
            all_rows, out_weight[layer_index], preferred_element_type=jnp.float32
        )
        partial_cols = lax.psum(partial_cols, "mp")
        projected = lax.all_to_all(partial_cols, "dp", split_axis=0, concat_axis=1, tiled=True)
        hidden = (hidden.astype(jnp.float32) + rms_scale(projected, post_gain[layer_index])).astype(
            jnp.bfloat16
        )
        keys_out.append(keys_new)
        values_out.append(value_new)
    return (hidden, jnp.stack(keys_out), jnp.stack(values_out))


MESH_ID = pl.DeviceIdType.MESH
BLOCK_ROWS = 8


def fits(mesh):
    parts = mesh.shape["mp"]
    query_heads = HEADS // parts
    key_heads = KV_HEADS // parts
    return (
        parts & (parts - 1) == 0
        and mesh.shape["dp"] & (mesh.shape["dp"] - 1) == 0
        and HEADS % parts == 0
        and KV_HEADS % parts == 0
        and query_heads == 2 * key_heads
        and query_heads + 2 * key_heads == BLOCK_ROWS
    )


def low(index, size):
    return index & (size - 1)


def high(index, size):
    return index >> (size.bit_length() - 1)


def one_hot(rows, columns, match):
    row = lax.broadcasted_iota(jnp.int32, (rows, columns), 0)
    column = lax.broadcasted_iota(jnp.int32, (rows, columns), 1)
    return jnp.where(match(row, column), 1.0, 0.0).astype(jnp.bfloat16)


def partners(mine, count):
    found = []
    for pattern in range(count):
        there = 0
        for bit in range(count.bit_length() - 1):
            held = lax.rem(mine // 2**bit, 2)
            there = there + 2**bit * (1 - held if pattern >> bit & 1 else held)
        found.append(there)
    return found


def pick(selector, values):
    return jnp.dot(selector, values, preferred_element_type=jnp.float32)


def fused_kernel(
    dp,
    mp,
    lengths_ref,
    windowed_ref,
    hidden_ref,
    in_gain_ref,
    post_gain_ref,
    query_hbm,
    key_hbm,
    value_hbm,
    out_hbm,
    key_cache_hbm,
    value_cache_hbm,
    hidden_out_ref,
    new_keys_ref,
    new_values_ref,
    query_w,
    key_w,
    value_w,
    out_w,
    keys,
    values,
    norm_send,
    norm_recv,
    proj_send,
    proj_recv,
    mix_send,
    mix_recv,
    cols_send,
    cols_recv,
    load_sem,
    send_sem,
    recv_sem,
):
    my_dp = lax.axis_index("dp")
    my_mp = lax.axis_index("mp")
    devices = dp * mp
    me = my_dp * mp + my_mp
    rows = hidden_ref.shape[0]
    total_rows = rows * dp
    slab = norm_send.shape[2]
    query_width = query_w.shape[1]
    key_width = key_w.shape[1]
    query_heads = query_width // HEAD_DIM
    key_heads = key_width // HEAD_DIM
    cache_rows = key_cache_hbm.shape[2]
    seq_block = cache_rows // KV_HEADS
    window_len = seq_block * mp // 2

    loads = [
        pltpu.make_async_copy(src, dst, load_sem.at[i])
        for i, (src, dst) in enumerate(
            (
                (query_hbm.at[0], query_w),
                (key_hbm.at[0], key_w),
                (value_hbm.at[0], value_w),
                (key_cache_hbm.at[0], keys),
                (value_cache_hbm.at[0], values),
                (out_hbm.at[0], out_w),
            )
        )
    ]
    peer_dp = partners(my_dp, dp)
    peer_mp = partners(my_mp, mp)
    others = [(i, j) for i in reversed(range(dp)) for j in reversed(range(mp)) if i + j > 0]
    barrier = pltpu.get_barrier_semaphore()
    for i, j in others:
        pl.semaphore_signal(
            barrier,
            inc=1,
            device_id={"dp": peer_dp[i], "mp": peer_mp[j]},
            device_id_type=MESH_ID,
        )
    for load in loads:
        load.start()

    hidden = hidden_ref[...].astype(jnp.float32)
    mean_square = jnp.mean(hidden * hidden, axis=-1, keepdims=True)
    normed = hidden * lax.rsqrt(mean_square + EPSILON) * in_gain_ref[...]
    for part in range(dp):
        norm_send[part] = normed[:, part * slab : (part + 1) * slab].astype(jnp.bfloat16)
    norm_recv[my_dp] = norm_send[my_dp]

    pl.semaphore_wait(barrier, devices - 1)
    for there in reversed(peer_dp[1:]):
        pltpu.make_async_remote_copy(
            src_ref=norm_send.at[there],
            dst_ref=norm_recv.at[my_dp],
            send_sem=send_sem.at[0],
            recv_sem=recv_sem.at[0],
            device_id={"dp": there, "mp": my_mp},
            device_id_type=MESH_ID,
        ).start()

    def finish(buffer, count, sem):
        block = buffer.at[pl.ds(0, count)]
        pltpu.make_async_copy(block, block, sem).wait()

    def scatter(send, recv, stage, slot_of):
        for i, j in others:
            there_dp = peer_dp[i]
            there_mp = peer_mp[j]
            pltpu.make_async_remote_copy(
                src_ref=send.at[slot_of(there_dp, there_mp)],
                dst_ref=recv.at[me],
                send_sem=send_sem.at[stage],
                recv_sem=recv_sem.at[stage],
                device_id={"dp": there_dp, "mp": there_mp},
                device_id_type=MESH_ID,
            ).start()
        recv[me] = send[slot_of(my_dp, my_mp)]

    lane = lax.broadcasted_iota(jnp.int32, (BLOCK_ROWS, HEAD_DIM), 1)
    half = HEAD_DIM // 2
    pair = jnp.where(lane < half, lane, lane - half).astype(jnp.float32)
    frequency = jnp.exp(pair * (-2.0 / HEAD_DIM * math.log(ROPE_BASE)))
    cosines = []
    sines = []
    for r in range(rows):
        angle = lengths_ref[r].astype(jnp.float32) * frequency
        cosines.append(jnp.cos(angle))
        sine = jnp.sin(angle)
        sines.append(jnp.where(lane < half, -sine, sine))

    for load in loads[:3]:
        load.wait()
    finish(norm_recv, dp - 1, recv_sem.at[0])
    tokens = jnp.concatenate(
        [norm_recv[part].astype(jnp.float32) for part in range(dp)], axis=0
    ).astype(jnp.bfloat16)
    parts = [
        jnp.dot(tokens, weight[...], preferred_element_type=jnp.float32)
        for weight in (query_w, key_w, value_w)
    ]
    pieces = []
    for part in parts:
        for at in range(0, part.shape[1], HEAD_DIM):
            pieces.append(part[:, at : at + HEAD_DIM])
    stacked = jnp.concatenate(pieces, axis=0).astype(jnp.bfloat16)
    spread = one_hot(
        total_rows * BLOCK_ROWS,
        total_rows * BLOCK_ROWS,
        lambda row, column: column
        == low(row, BLOCK_ROWS) * total_rows + high(row, BLOCK_ROWS),
    )
    proj_send[...] = (
        pick(spread, stacked).astype(jnp.bfloat16).reshape(dp, rows * BLOCK_ROWS, HEAD_DIM)
    )
    scatter(proj_send, proj_recv, 1, lambda there_dp, there_mp: there_dp)

    for load in loads[3:5]:
        load.wait()
    group_rows = mp * BLOCK_ROWS
    row = lax.broadcasted_iota(jnp.int32, (group_rows, cache_rows), 0)
    column = lax.broadcasted_iota(jnp.int32, (group_rows, cache_rows), 1)
    in_block = low(row, BLOCK_ROWS)
    head_match = (in_block < query_heads) & (
        low(column, KV_HEADS) == high(row, BLOCK_ROWS) * key_heads + high(in_block, 2)
    )
    position = my_mp * seq_block + high(column, KV_HEADS)
    allowed = []
    for r in range(rows):
        length = lengths_ref[r]
        floor = jnp.where(windowed_ref[0, r] == 0, -1, length - window_len)
        allowed.append(head_match & (position < length) & (position > floor))
    self_row = lax.broadcasted_iota(jnp.int32, (group_rows, group_rows), 0)
    self_column = lax.broadcasted_iota(jnp.int32, (group_rows, group_rows), 1)
    self_slot = low(self_row, BLOCK_ROWS)
    own_base = self_row - self_slot + query_heads + high(self_slot, 2)
    is_query = self_slot < query_heads
    self_key = is_query & (self_column == own_base)
    self_value = jnp.where(is_query & (self_column == own_base + key_heads), 1.0, 0.0).astype(
        jnp.bfloat16
    )
    acc_row = low(lax.broadcasted_iota(jnp.int32, (group_rows, HEAD_DIM), 0), BLOCK_ROWS)
    self_share = jnp.where(my_mp == 0, 1.0, 0.0)

    finish(proj_recv, devices - 1, recv_sem.at[1])
    blocks = rows * BLOCK_ROWS
    summed = jnp.sum(
        proj_recv[...].astype(jnp.float32).reshape(dp, mp, blocks, HEAD_DIM), axis=0
    )
    rotated_rows = []
    raw_rows = []
    for r in range(rows):
        raw = summed[:, r * BLOCK_ROWS : (r + 1) * BLOCK_ROWS, :].reshape(group_rows, HEAD_DIM)
        raw = raw.astype(jnp.bfloat16)
        wide = raw.astype(jnp.float32)
        cosine = jnp.concatenate([cosines[r]] * mp, axis=0)
        sine = jnp.concatenate([sines[r]] * mp, axis=0)
        turned = wide * cosine + pltpu.roll(wide, half, 1) * sine
        queries = (turned * HEAD_DIM ** (-0.5)).astype(jnp.bfloat16)
        turned = turned.astype(jnp.bfloat16)
        rotated_rows.append(turned)
        raw_rows.append(raw)
        flat_keys = keys[r]
        flat_values = values[r]
        over_last = (((1,), (1,)), ((), ()))
        scores = lax.dot_general(
            queries, flat_keys, over_last, preferred_element_type=jnp.float32
        )
        scores = SOFTCAP * jnp.tanh(scores * (1.0 / SOFTCAP))
        exp_scores = jnp.where(allowed[r], jnp.exp(scores), 0.0)
        sums_exp = jnp.sum(exp_scores, axis=-1, keepdims=True)
        accumulated = jnp.dot(
            exp_scores.astype(jnp.bfloat16), flat_values, preferred_element_type=jnp.float32
        )
        own = lax.dot_general(queries, turned, over_last, preferred_element_type=jnp.float32)
        own = jnp.sum(jnp.where(self_key, own, 0.0), axis=-1, keepdims=True)
        own = jnp.exp(SOFTCAP * jnp.tanh(own * (1.0 / SOFTCAP))) * self_share
        accumulated = accumulated + own * pick(self_value, raw)
        sums_exp = jnp.broadcast_to(sums_exp + own, (group_rows, HEAD_DIM))
        message = jnp.where(
            acc_row < query_heads, accumulated, pltpu.roll(sums_exp, query_heads, 0)
        )
        mix_send[:, r * BLOCK_ROWS : (r + 1) * BLOCK_ROWS, :] = message.reshape(
            mp, BLOCK_ROWS, HEAD_DIM
        ).astype(mix_send.dtype)
    scatter(mix_send, mix_recv, 2, lambda there_dp, there_mp: there_mp)

    turned_all = jnp.concatenate(rotated_rows, axis=0)
    raw_all = jnp.concatenate(raw_rows, axis=0)

    def owner(row, first):
        head = low(row, KV_HEADS)
        return (
            high(row, KV_HEADS) * group_rows
            + high(head, key_heads) * BLOCK_ROWS
            + first
            + low(head, key_heads)
        )

    key_rows = one_hot(
        rows * KV_HEADS, rows * group_rows, lambda row, column: column == owner(row, query_heads)
    )
    value_rows = one_hot(
        rows * KV_HEADS,
        rows * group_rows,
        lambda row, column: column == owner(row, query_heads + key_heads),
    )
    new_keys_ref[...] = (
        pick(key_rows, turned_all).astype(jnp.bfloat16).reshape(new_keys_ref.shape)
    )
    new_values_ref[...] = (
        pick(value_rows, raw_all).astype(jnp.bfloat16).reshape(new_values_ref.shape)
    )
    gather = one_hot(
        query_heads * total_rows,
        total_rows * BLOCK_ROWS,
        lambda row, column: column
        == low(row, total_rows) * BLOCK_ROWS + high(row, total_rows),
    )

    loads[5].wait()
    finish(mix_recv, devices - 1, recv_sem.at[2])
    mixed = jnp.sum(
        mix_recv[...].astype(jnp.float32).reshape(dp, mp, blocks, HEAD_DIM), axis=1
    ).reshape(dp * blocks, HEAD_DIM)
    all_row = low(lax.broadcasted_iota(jnp.int32, mixed.shape, 0), BLOCK_ROWS)
    weights = pltpu.roll(mixed, mixed.shape[0] - query_heads, 0)
    attended = jnp.where(all_row < query_heads, mixed / weights, 0.0).astype(jnp.bfloat16)
    heads = pick(gather, attended).astype(jnp.bfloat16)
    heads = jnp.concatenate(
        [heads[b * total_rows : (b + 1) * total_rows] for b in range(query_heads)], axis=1
    )
    partial_cols = lax.dot_general(
        heads, out_w[...], over_last, preferred_element_type=jnp.float32
    )
    for part in range(dp):
        cols_send[part] = partial_cols[part * rows : (part + 1) * rows].astype(cols_send.dtype)
    scatter(cols_send, cols_recv, 3, lambda there_dp, there_mp: there_dp)
    finish(cols_recv, devices - 1, recv_sem.at[3])
    pieces = []
    for part in range(dp):
        piece = cols_recv[part * mp].astype(jnp.float32)
        for other in range(1, mp):
            piece = piece + cols_recv[part * mp + other].astype(jnp.float32)
        pieces.append(piece)
    projected = jnp.concatenate(pieces, axis=1)
    mean_square = jnp.mean(projected * projected, axis=-1, keepdims=True)
    update = projected * lax.rsqrt(mean_square + EPSILON) * post_gain_ref[...]
    hidden_out_ref[...] = (hidden_ref[...].astype(jnp.float32) + update).astype(jnp.bfloat16)

    finish(norm_recv, dp - 1, send_sem.at[0])
    finish(proj_recv, devices - 1, send_sem.at[1])
    finish(mix_recv, devices - 1, send_sem.at[2])
    finish(cols_recv, devices - 1, send_sem.at[3])


def copy_kernel(a_ref, b_ref, c_ref, a_out, b_out, c_out):
    a_out[...] = a_ref[...]
    b_out[...] = b_ref[...]
    c_out[...] = c_ref[...]


def fused_device(
    hidden,
    in_gain,
    post_gain,
    query_weight,
    key_weight,
    value_weight,
    out_weight,
    key_cache,
    value_cache,
    lengths,
    windowed,
):
    dp = lax.axis_size("dp")
    mp = lax.axis_size("mp")
    rows = hidden.shape[0]
    slab = query_weight.shape[1]
    out_slab = out_weight.shape[2]
    blocks = rows * BLOCK_ROWS
    half_word = jnp.bfloat16
    flat = (LAYERS, rows, key_cache.shape[2] * KV_HEADS, HEAD_DIM)
    out_shape = (
        jax.ShapeDtypeStruct(hidden.shape, half_word),
        jax.ShapeDtypeStruct((LAYERS, rows, KV_HEADS, HEAD_DIM), half_word),
        jax.ShapeDtypeStruct((LAYERS, rows, KV_HEADS, HEAD_DIM), half_word),
    )
    smem = pl.BlockSpec(memory_space=pltpu.SMEM)
    vmem = pl.BlockSpec(memory_space=pltpu.VMEM)
    far = pl.BlockSpec(memory_space=pl.ANY)
    results = pl.pallas_call(
        functools.partial(fused_kernel, dp, mp),
        out_shape=out_shape,
        in_specs=[smem, smem, vmem, vmem, vmem, far, far, far, far, far, far],
        out_specs=(vmem, vmem, vmem),
        scratch_shapes=[
            pltpu.VMEM(query_weight.shape[1:], half_word),
            pltpu.VMEM(key_weight.shape[1:], half_word),
            pltpu.VMEM(value_weight.shape[1:], half_word),
            pltpu.VMEM((out_slab, out_weight.shape[1]), half_word),
            pltpu.VMEM(flat[1:], half_word),
            pltpu.VMEM(flat[1:], half_word),
            pltpu.VMEM((dp, rows, slab), half_word),
            pltpu.VMEM((dp, rows, slab), half_word),
            pltpu.VMEM((dp, blocks, HEAD_DIM), half_word),
            pltpu.VMEM((dp * mp, blocks, HEAD_DIM), half_word),
            pltpu.VMEM((mp, blocks, HEAD_DIM), half_word),
            pltpu.VMEM((dp * mp, blocks, HEAD_DIM), half_word),
            pltpu.VMEM((dp, rows, out_slab), half_word),
            pltpu.VMEM((dp * mp, rows, out_slab), half_word),
            pltpu.SemaphoreType.DMA((6,)),
            pltpu.SemaphoreType.DMA((4,)),
            pltpu.SemaphoreType.DMA((4,)),
        ],
        compiler_params=pltpu.CompilerParams(collective_id=0, has_side_effects=True),
    )(
        lengths,
        windowed,
        hidden,
        in_gain,
        post_gain,
        query_weight,
        key_weight,
        value_weight,
        jnp.swapaxes(out_weight, 1, 2),
        key_cache.reshape(flat),
        value_cache.reshape(flat),
    )
    plain = pl.pallas_call(copy_kernel, out_shape=out_shape, in_specs=[vmem] * 3, out_specs=(vmem,) * 3)
    return plain(*results)


def solution(mesh):
    return jax.shard_map(
        fused_device if fits(mesh) else on_device,
        mesh=mesh,
        in_specs=(
            P("dp", None),
            P(),
            P(),
            P(None, "dp", "mp"),
            P(None, "dp", "mp"),
            P(None, "dp", "mp"),
            P(None, "mp", "dp"),
            P(None, "dp", "mp", None, None),
            P(None, "dp", "mp", None, None),
            P("dp"),
            P(None, "dp"),
        ),
        out_specs=(P("dp", None), P(None, "dp", None, None), P(None, "dp", None, None)),
        check_vma=False,
    )
```

```python
import functools
import math

import jax
import jax.numpy as jnp
from jax import lax
from jax.experimental import pallas as pl
from jax.experimental.pallas import tpu as pltpu
from jax.sharding import PartitionSpec as P

HEADS = 16
KV_HEADS = 8
HEAD_DIM = 128
LAYERS = 1


EPSILON = 1e-06
SOFTCAP = 50.0
ROPE_BASE = 10000.0
NEGATIVE = -1e30


def rms_scale(values, gain_row):
    values = values.astype(jnp.float32)
    mean_square = jnp.mean(values * values, axis=-1, keepdims=True)
    return values * lax.rsqrt(mean_square + EPSILON) * gain_row.astype(jnp.float32)


def rotate(values, positions):
    half_dim = values.shape[-1] // 2
    frequency = jnp.power(
        ROPE_BASE, -2.0 * jnp.arange(half_dim, dtype=jnp.float32) / values.shape[-1]
    )
    angles = positions.astype(jnp.float32)[:, None] * frequency[None, :]
    cosine = jnp.cos(angles)[:, None, :]
    sine_table = jnp.sin(angles)[:, None, :]
    front_half = values[..., :half_dim]
    back_half = values[..., half_dim:]
    return jnp.concatenate(
        (
            front_half * cosine - back_half * sine_table,
            back_half * cosine + front_half * sine_table,
        ),
        axis=-1,
    )


def on_device(
    hidden,
    in_gain,
    post_gain,
    query_weight,
    key_weight,
    value_weight,
    out_weight,
    key_cache,
    value_cache,
    lengths,
    windowed,
):
    row_count = hidden.shape[0]
    query_width = query_weight.shape[2]
    key_width = key_weight.shape[2]
    seq_block = key_cache.shape[2]
    head_width = out_weight.shape[1]
    group_size = HEADS // KV_HEADS
    window_len = seq_block * lax.axis_size("mp") // 2
    keys_out = []
    values_out = []
    for layer_index in range(LAYERS):
        normed = rms_scale(hidden, in_gain[layer_index]).astype(jnp.bfloat16)
        token_slab = lax.all_to_all(normed, "dp", split_axis=1, concat_axis=0, tiled=True)
        joined = jnp.concatenate(
            (query_weight[layer_index], key_weight[layer_index], value_weight[layer_index]), 1
        )

        def local_term():
            part_rows = lax.slice_in_dim(token_slab, 0, row_count * lax.axis_size("dp"), axis=0)
            return jnp.dot(part_rows, joined, preferred_element_type=jnp.float32)

        summed = lax.psum_scatter(local_term(), "dp", scatter_dimension=0, tiled=True)
        query_part = summed[:, :query_width]
        key_part = summed[:, query_width : query_width + key_width]
        value_part = summed[:, query_width + key_width :]
        rounded = (
            query_part.astype(jnp.bfloat16),
            key_part.astype(jnp.bfloat16),
            value_part.astype(jnp.bfloat16),
        )
        query, key_raw, value_new = (
            lax.all_gather(rounded[0], "mp", axis=1, tiled=True),
            lax.all_gather(rounded[1], "mp", axis=1, tiled=True),
            lax.all_gather(rounded[2], "mp", axis=1, tiled=True),
        )
        queries = rotate(query.astype(jnp.float32).reshape(row_count, HEADS, HEAD_DIM), lengths)
        queries = (queries * HEAD_DIM ** (-0.5)).astype(jnp.bfloat16)
        keys_new = rotate(
            key_raw.astype(jnp.float32).reshape(row_count, KV_HEADS, HEAD_DIM), lengths
        ).astype(jnp.bfloat16)
        value_new = value_new.reshape(row_count, KV_HEADS, HEAD_DIM)
        grouped = queries.reshape(row_count, KV_HEADS, group_size, HEAD_DIM)
        scores = jnp.einsum(
            "rkgd,rskd->rkgs", grouped, key_cache[layer_index], preferred_element_type=jnp.float32
        )
        scores = SOFTCAP * jnp.tanh(scores / SOFTCAP)
        positions = lax.axis_index("mp") * seq_block + jnp.arange(seq_block, dtype=jnp.int32)
        window_flag = windowed[layer_index][:, None]
        usable = (positions[None, :] < lengths[:, None]) & (
            (window_flag == 0) | (positions[None, :] > lengths[:, None] - window_len)
        )
        usable = usable[:, None, None, :]
        masked = jnp.where(usable, scores, NEGATIVE)
        peaks = jnp.max(masked, axis=-1)
        exp_scores = jnp.where(usable, jnp.exp(masked - peaks[..., None]), 0.0)
        sums_exp = jnp.sum(exp_scores, axis=-1)
        accumulated = jnp.einsum(
            "rkgs,rskd->rkgd",
            exp_scores,
            value_cache[layer_index].astype(jnp.float32),
            preferred_element_type=jnp.float32,
        )
        global_peak = lax.pmax(peaks, "mp")
        rescale = jnp.exp(peaks - global_peak)
        sums_exp, accumulated = lax.psum(
            (sums_exp * rescale, accumulated * rescale[..., None]), "mp"
        )
        peaks = global_peak
        self_score = jnp.einsum(
            "rkgd,rkd->rkg", grouped, keys_new, preferred_element_type=jnp.float32
        )
        self_score = SOFTCAP * jnp.tanh(self_score / SOFTCAP)
        peak_all = jnp.maximum(peaks, self_score)
        old_scale = jnp.exp(peaks - peak_all)
        self_weight = jnp.exp(self_score - peak_all)
        denominator = sums_exp * old_scale + self_weight
        mixed = (
            accumulated * old_scale[..., None]
            + self_weight[..., None] * value_new.astype(jnp.float32)[:, :, None, :]
        )
        attended = (
            (mixed / denominator[..., None])
            .reshape(row_count, HEADS * HEAD_DIM)
            .astype(jnp.bfloat16)
        )
        attended_local = lax.dynamic_slice_in_dim(
            attended, lax.axis_index("mp") * head_width, head_width, 1
        )
        all_rows = lax.all_gather(attended_local, "dp", axis=0, tiled=True)
        partial_cols = jnp.dot(
            all_rows, out_weight[layer_index], preferred_element_type=jnp.float32
        )
        partial_cols = lax.psum(partial_cols, "mp")
        projected = lax.all_to_all(partial_cols, "dp", split_axis=0, concat_axis=1, tiled=True)
        hidden = (hidden.astype(jnp.float32) + rms_scale(projected, post_gain[layer_index])).astype(
            jnp.bfloat16
        )
        keys_out.append(keys_new)
        values_out.append(value_new)
    return (hidden, jnp.stack(keys_out), jnp.stack(values_out))


MESH_ID = pl.DeviceIdType.MESH
BLOCK_ROWS = 8


def fits(mesh):
    parts = mesh.shape["mp"]
    query_heads = HEADS // parts
    key_heads = KV_HEADS // parts
    return (
        parts & (parts - 1) == 0
        and mesh.shape["dp"] & (mesh.shape["dp"] - 1) == 0
        and HEADS % parts == 0
        and KV_HEADS % parts == 0
        and query_heads == 2 * key_heads
        and query_heads + 2 * key_heads == BLOCK_ROWS
    )


def low(index, size):
    return index & (size - 1)


def high(index, size):
    return index >> (size.bit_length() - 1)


def one_hot(rows, columns, match):
    row = lax.broadcasted_iota(jnp.int32, (rows, columns), 0)
    column = lax.broadcasted_iota(jnp.int32, (rows, columns), 1)
    return jnp.where(match(row, column), 1.0, 0.0).astype(jnp.bfloat16)


def partners(mine, count):
    found = []
    for pattern in range(count):
        there = 0
        for bit in range(count.bit_length() - 1):
            held = lax.rem(mine // 2**bit, 2)
            there = there + 2**bit * (1 - held if pattern >> bit & 1 else held)
        found.append(there)
    return found


def pick(selector, values):
    return jnp.dot(selector, values, preferred_element_type=jnp.float32)


def fused_kernel(
    dp,
    mp,
    lengths_hbm,
    windowed_hbm,
    hidden_hbm,
    in_gain_hbm,
    post_gain_hbm,
    query_hbm,
    key_hbm,
    value_hbm,
    out_hbm,
    key_cache_hbm,
    value_cache_hbm,
    hidden_out_ref,
    new_keys_ref,
    new_values_ref,
    lengths_ref,
    windowed_ref,
    hidden_ref,
    in_gain_ref,
    post_gain_ref,
    query_w,
    key_w,
    value_w,
    out_w,
    keys,
    values,
    norm_send,
    norm_recv,
    proj_send,
    proj_recv,
    whole_send,
    whole_recv,
    mix_send,
    mix_recv,
    heads_send,
    heads_recv,
    cols_send,
    cols_recv,
    load_sem,
    send_sem,
    recv_sem,
):
    my_dp = lax.axis_index("dp")
    my_mp = lax.axis_index("mp")
    devices = dp * mp
    me = my_dp * mp + my_mp
    rows = hidden_ref.shape[0]
    total_rows = rows * dp
    slab = norm_send.shape[2]
    query_width = query_w.shape[1]
    key_width = key_w.shape[1]
    query_heads = query_width // HEAD_DIM
    key_heads = key_width // HEAD_DIM
    cache_rows = key_cache_hbm.shape[2]
    seq_block = cache_rows // KV_HEADS
    window_len = seq_block * mp // 2

    loads = [
        pltpu.make_async_copy(src, dst, load_sem.at[i])
        for i, (src, dst) in enumerate(
            (
                (hidden_hbm, hidden_ref),
                (in_gain_hbm, in_gain_ref),
                (lengths_hbm, lengths_ref),
                (windowed_hbm, windowed_ref),
                (query_hbm.at[0], query_w),
                (key_hbm.at[0], key_w),
                (value_hbm.at[0], value_w),
                (key_cache_hbm.at[0], keys),
                (value_cache_hbm.at[0], values),
                (out_hbm.at[0], out_w),
                (post_gain_hbm, post_gain_ref),
            )
        )
    ]
    peer_dp = partners(my_dp, dp)
    peer_mp = partners(my_mp, mp)
    others = [(i, j) for i in reversed(range(dp)) for j in reversed(range(mp)) if i + j > 0]
    barrier = pltpu.get_barrier_semaphore()
    near = [(i, j) for i, j in others if i == 0 or j == 0]
    for i, j in near:
        pl.semaphore_signal(
            barrier,
            inc=1,
            device_id={"dp": peer_dp[i], "mp": peer_mp[j]},
            device_id_type=MESH_ID,
        )
    for load in loads:
        load.start()
    for load in loads[:2]:
        load.wait()

    hidden = hidden_ref[...].astype(jnp.float32)
    mean_square = jnp.mean(hidden * hidden, axis=-1, keepdims=True)
    normed = hidden * lax.rsqrt(mean_square + EPSILON) * in_gain_ref[...]
    for part in range(dp):
        norm_send[part] = normed[:, part * slab : (part + 1) * slab].astype(jnp.bfloat16)

    pl.semaphore_wait(barrier, len(near))
    def finish(buffer, count, sem):
        block = buffer.at[pl.ds(0, count)]
        pltpu.make_async_copy(block, block, sem).wait()

    def exchange(recv, stage, targets, source, slot):
        for i, j in targets:
            pltpu.make_async_remote_copy(
                src_ref=source(peer_dp[i], peer_mp[j]),
                dst_ref=recv.at[slot],
                send_sem=send_sem.at[stage],
                recv_sem=recv_sem.at[stage],
                device_id={"dp": peer_dp[i], "mp": peer_mp[j]},
                device_id_type=MESH_ID,
            ).start()

    along_dp = [(i, j) for i, j in near if j == 0]
    along_mp = [(i, j) for i, j in near if i == 0]
    exchange(norm_recv, 0, along_dp, lambda a, b: norm_send.at[a], my_dp)
    norm_recv[my_dp] = norm_send[my_dp]
    for load in loads[2:4]:
        load.wait()

    lane = lax.broadcasted_iota(jnp.int32, (BLOCK_ROWS, HEAD_DIM), 1)
    half = HEAD_DIM // 2
    pair = jnp.where(lane < half, lane, lane - half).astype(jnp.float32)
    frequency = jnp.exp(pair * (-2.0 / HEAD_DIM * math.log(ROPE_BASE)))
    cosines = []
    sines = []
    for r in range(rows):
        angle = lengths_ref[r].astype(jnp.float32) * frequency
        cosines.append(jnp.cos(angle))
        sine = jnp.sin(angle)
        sines.append(jnp.where(lane < half, -sine, sine))

    for load in loads[4:7]:
        load.wait()
    finish(norm_recv, dp - 1, recv_sem.at[0])
    tokens = jnp.concatenate(
        [norm_recv[part].astype(jnp.float32) for part in range(dp)], axis=0
    ).astype(jnp.bfloat16)
    parts = [
        jnp.dot(tokens, weight[...], preferred_element_type=jnp.float32)
        for weight in (query_w, key_w, value_w)
    ]
    pieces = []
    for part in parts:
        for at in range(0, part.shape[1], HEAD_DIM):
            pieces.append(part[:, at : at + HEAD_DIM])
    stacked = jnp.concatenate(pieces, axis=0).astype(jnp.bfloat16)
    spread = one_hot(
        total_rows * BLOCK_ROWS,
        total_rows * BLOCK_ROWS,
        lambda row, column: column
        == low(row, BLOCK_ROWS) * total_rows + high(row, BLOCK_ROWS),
    )
    proj_send[...] = (
        pick(spread, stacked).astype(jnp.bfloat16).reshape(dp, rows * BLOCK_ROWS, HEAD_DIM)
    )
    exchange(proj_recv, 1, along_dp, lambda a, b: proj_send.at[a], my_dp)
    proj_recv[my_dp] = proj_send[my_dp]

    for load in loads[7:9]:
        load.wait()
    group_rows = mp * BLOCK_ROWS
    row = lax.broadcasted_iota(jnp.int32, (group_rows, cache_rows), 0)
    column = lax.broadcasted_iota(jnp.int32, (group_rows, cache_rows), 1)
    in_block = low(row, BLOCK_ROWS)
    head_match = (in_block < query_heads) & (
        low(column, KV_HEADS) == high(row, BLOCK_ROWS) * key_heads + high(in_block, 2)
    )
    position = my_mp * seq_block + high(column, KV_HEADS)
    allowed = []
    for r in range(rows):
        length = lengths_ref[r]
        floor = jnp.where(windowed_ref[0, r] == 0, -1, length - window_len)
        allowed.append(head_match & (position < length) & (position > floor))
    self_row = lax.broadcasted_iota(jnp.int32, (group_rows, group_rows), 0)
    self_column = lax.broadcasted_iota(jnp.int32, (group_rows, group_rows), 1)
    self_slot = low(self_row, BLOCK_ROWS)
    own_base = self_row - self_slot + query_heads + high(self_slot, 2)
    is_query = self_slot < query_heads
    self_key = is_query & (self_column == own_base)
    self_value = jnp.where(is_query & (self_column == own_base + key_heads), 1.0, 0.0).astype(
        jnp.bfloat16
    )
    acc_row = low(lax.broadcasted_iota(jnp.int32, (group_rows, HEAD_DIM), 0), BLOCK_ROWS)
    self_share = jnp.where(my_mp == 0, 1.0, 0.0)

    finish(proj_recv, dp - 1, recv_sem.at[1])
    blocks = rows * BLOCK_ROWS
    whole_send[...] = jnp.sum(proj_recv[...].astype(jnp.float32), axis=0).astype(jnp.bfloat16)
    exchange(whole_recv, 2, along_mp, lambda a, b: whole_send, my_mp)
    whole_recv[my_mp] = whole_send[...]
    finish(whole_recv, mp - 1, recv_sem.at[2])
    summed = whole_recv[...].astype(jnp.float32)
    rotated_rows = []
    raw_rows = []
    for r in range(rows):
        raw = summed[:, r * BLOCK_ROWS : (r + 1) * BLOCK_ROWS, :].reshape(group_rows, HEAD_DIM)
        raw = raw.astype(jnp.bfloat16)
        wide = raw.astype(jnp.float32)
        cosine = jnp.concatenate([cosines[r]] * mp, axis=0)
        sine = jnp.concatenate([sines[r]] * mp, axis=0)
        turned = wide * cosine + pltpu.roll(wide, half, 1) * sine
        queries = (turned * HEAD_DIM ** (-0.5)).astype(jnp.bfloat16)
        turned = turned.astype(jnp.bfloat16)
        rotated_rows.append(turned)
        raw_rows.append(raw)
        flat_keys = keys[r]
        flat_values = values[r]
        over_last = (((1,), (1,)), ((), ()))
        scores = lax.dot_general(
            queries, flat_keys, over_last, preferred_element_type=jnp.float32
        )
        scores = SOFTCAP * jnp.tanh(scores * (1.0 / SOFTCAP))
        exp_scores = jnp.where(allowed[r], jnp.exp(scores), 0.0)
        sums_exp = jnp.sum(exp_scores, axis=-1, keepdims=True)
        accumulated = jnp.dot(
            exp_scores.astype(jnp.bfloat16), flat_values, preferred_element_type=jnp.float32
        )
        own = lax.dot_general(queries, turned, over_last, preferred_element_type=jnp.float32)
        own = jnp.sum(jnp.where(self_key, own, 0.0), axis=-1, keepdims=True)
        own = jnp.exp(SOFTCAP * jnp.tanh(own * (1.0 / SOFTCAP))) * self_share
        accumulated = accumulated + own * pick(self_value, raw)
        sums_exp = jnp.broadcast_to(sums_exp + own, (group_rows, HEAD_DIM))
        message = jnp.where(
            acc_row < query_heads, accumulated, pltpu.roll(sums_exp, query_heads, 0)
        )
        mix_send[:, r * BLOCK_ROWS : (r + 1) * BLOCK_ROWS, :] = message.reshape(
            mp, BLOCK_ROWS, HEAD_DIM
        ).astype(mix_send.dtype)
    exchange(mix_recv, 3, along_mp, lambda a, b: mix_send.at[b], my_mp)
    mix_recv[my_mp] = mix_send[my_mp]

    finish(mix_recv, mp - 1, recv_sem.at[3])
    mixed = jnp.sum(mix_recv[...].astype(jnp.float32), axis=0)
    attended = []
    for r in range(rows):
        at = r * BLOCK_ROWS
        attended.append(
            mixed[at : at + query_heads] / mixed[at + query_heads : at + 2 * query_heads]
        )
    heads_send[...] = jnp.concatenate(attended, axis=0).astype(jnp.bfloat16)
    exchange(heads_recv, 4, along_dp, lambda a, b: heads_send, my_dp)
    heads_recv[my_dp] = heads_send[...]
    turned_all = jnp.concatenate(rotated_rows, axis=0)
    raw_all = jnp.concatenate(raw_rows, axis=0)

    def owner(row, first):
        head = low(row, KV_HEADS)
        return (
            high(row, KV_HEADS) * group_rows
            + high(head, key_heads) * BLOCK_ROWS
            + first
            + low(head, key_heads)
        )

    key_rows = one_hot(
        rows * KV_HEADS, rows * group_rows, lambda row, column: column == owner(row, query_heads)
    )
    value_rows = one_hot(
        rows * KV_HEADS,
        rows * group_rows,
        lambda row, column: column == owner(row, query_heads + key_heads),
    )
    new_keys_ref[...] = (
        pick(key_rows, turned_all).astype(jnp.bfloat16).reshape(new_keys_ref.shape)
    )
    new_values_ref[...] = (
        pick(value_rows, raw_all).astype(jnp.bfloat16).reshape(new_values_ref.shape)
    )
    gather = one_hot(
        query_heads * total_rows,
        query_heads * total_rows,
        lambda row, column: column
        == low(row, total_rows) * query_heads + high(row, total_rows),
    )
    for load in loads[9:]:
        load.wait()
    finish(heads_recv, dp - 1, recv_sem.at[4])
    attended = heads_recv[...].astype(jnp.float32).reshape(total_rows * query_heads, HEAD_DIM)
    heads = pick(gather, attended.astype(jnp.bfloat16)).astype(jnp.bfloat16)
    heads = jnp.concatenate(
        [heads[b * total_rows : (b + 1) * total_rows] for b in range(query_heads)], axis=1
    )
    partial_cols = lax.dot_general(
        heads, out_w[...], over_last, preferred_element_type=jnp.float32
    )
    for part in range(dp):
        cols_send[part] = partial_cols[part * rows : (part + 1) * rows].astype(cols_send.dtype)
    exchange(cols_recv, 5, others, lambda a, b: cols_send.at[a], me)
    cols_recv[me] = cols_send[my_dp]
    finish(cols_recv, devices - 1, recv_sem.at[5])
    pieces = []
    for part in range(dp):
        piece = cols_recv[part * mp].astype(jnp.float32)
        for other in range(1, mp):
            piece = piece + cols_recv[part * mp + other].astype(jnp.float32)
        pieces.append(piece)
    projected = jnp.concatenate(pieces, axis=1)
    mean_square = jnp.mean(projected * projected, axis=-1, keepdims=True)
    update = projected * lax.rsqrt(mean_square + EPSILON) * post_gain_ref[...]
    hidden_out_ref[...] = (hidden_ref[...].astype(jnp.float32) + update).astype(jnp.bfloat16)

    finish(norm_recv, dp - 1, send_sem.at[0])
    finish(proj_recv, dp - 1, send_sem.at[1])
    finish(whole_recv, mp - 1, send_sem.at[2])
    finish(mix_recv, mp - 1, send_sem.at[3])
    finish(heads_recv, dp - 1, send_sem.at[4])
    finish(cols_recv, devices - 1, send_sem.at[5])


def copy_kernel(a_ref, b_ref, c_ref, a_out, b_out, c_out):
    a_out[...] = a_ref[...]
    b_out[...] = b_ref[...]
    c_out[...] = c_ref[...]


def fused_device(
    hidden,
    in_gain,
    post_gain,
    query_weight,
    key_weight,
    value_weight,
    out_weight,
    key_cache,
    value_cache,
    lengths,
    windowed,
):
    dp = lax.axis_size("dp")
    mp = lax.axis_size("mp")
    rows = hidden.shape[0]
    slab = query_weight.shape[1]
    out_slab = out_weight.shape[2]
    blocks = rows * BLOCK_ROWS
    half_word = jnp.bfloat16
    flat = (LAYERS, rows, key_cache.shape[2] * KV_HEADS, HEAD_DIM)
    out_shape = (
        jax.ShapeDtypeStruct(hidden.shape, half_word),
        jax.ShapeDtypeStruct((LAYERS, rows, KV_HEADS, HEAD_DIM), half_word),
        jax.ShapeDtypeStruct((LAYERS, rows, KV_HEADS, HEAD_DIM), half_word),
    )
    vmem = pl.BlockSpec(memory_space=pltpu.VMEM)
    far = pl.BlockSpec(memory_space=pl.ANY)
    results = pl.pallas_call(
        functools.partial(fused_kernel, dp, mp),
        out_shape=out_shape,
        in_specs=[far] * 11,
        out_specs=(vmem, vmem, vmem),
        scratch_shapes=[
            pltpu.SMEM(lengths.shape, lengths.dtype),
            pltpu.SMEM(windowed.shape, windowed.dtype),
            pltpu.VMEM(hidden.shape, hidden.dtype),
            pltpu.VMEM(in_gain.shape, in_gain.dtype),
            pltpu.VMEM(post_gain.shape, post_gain.dtype),
            pltpu.VMEM(query_weight.shape[1:], half_word),
            pltpu.VMEM(key_weight.shape[1:], half_word),
            pltpu.VMEM(value_weight.shape[1:], half_word),
            pltpu.VMEM((out_slab, out_weight.shape[1]), half_word),
            pltpu.VMEM(flat[1:], half_word),
            pltpu.VMEM(flat[1:], half_word),
            pltpu.VMEM((dp, rows, slab), half_word),
            pltpu.VMEM((dp, rows, slab), half_word),
            pltpu.VMEM((dp, blocks, HEAD_DIM), half_word),
            pltpu.VMEM((dp, blocks, HEAD_DIM), half_word),
            pltpu.VMEM((blocks, HEAD_DIM), half_word),
            pltpu.VMEM((mp, blocks, HEAD_DIM), half_word),
            pltpu.VMEM((mp, blocks, HEAD_DIM), half_word),
            pltpu.VMEM((mp, blocks, HEAD_DIM), half_word),
            pltpu.VMEM((rows * out_weight.shape[1] // HEAD_DIM, HEAD_DIM), half_word),
            pltpu.VMEM((dp, rows * out_weight.shape[1] // HEAD_DIM, HEAD_DIM), half_word),
            pltpu.VMEM((dp, rows, out_slab), half_word),
            pltpu.VMEM((dp * mp, rows, out_slab), half_word),
            pltpu.SemaphoreType.DMA((11,)),
            pltpu.SemaphoreType.DMA((6,)),
            pltpu.SemaphoreType.DMA((6,)),
        ],
        compiler_params=pltpu.CompilerParams(collective_id=0, has_side_effects=True),
    )(
        lengths,
        windowed,
        hidden,
        in_gain,
        post_gain,
        query_weight,
        key_weight,
        value_weight,
        jnp.swapaxes(out_weight, 1, 2),
        key_cache.reshape(flat),
        value_cache.reshape(flat),
    )
    plain = pl.pallas_call(copy_kernel, out_shape=out_shape, in_specs=[vmem] * 3, out_specs=(vmem,) * 3)
    return plain(*results)


def solution(mesh):
    return jax.shard_map(
        fused_device if fits(mesh) else on_device,
        mesh=mesh,
        in_specs=(
            P("dp", None),
            P(),
            P(),
            P(None, "dp", "mp"),
            P(None, "dp", "mp"),
            P(None, "dp", "mp"),
            P(None, "mp", "dp"),
            P(None, "dp", "mp", None, None),
            P(None, "dp", "mp", None, None),
            P("dp"),
            P(None, "dp"),
        ),
        out_specs=(P("dp", None), P(None, "dp", None, None), P(None, "dp", None, None)),
        check_vma=False,
    )
```

```python
import functools
import math

import jax
import jax.numpy as jnp
from jax import lax
from jax.experimental import pallas as pl
from jax.experimental.pallas import tpu as pltpu
from jax.sharding import PartitionSpec as P

HEADS = 16
KV_HEADS = 8
HEAD_DIM = 128
LAYERS = 1


EPSILON = 1e-06
SOFTCAP = 50.0
ROPE_BASE = 10000.0
NEGATIVE = -1e30


def rms_scale(values, gain_row):
    values = values.astype(jnp.float32)
    mean_square = jnp.mean(values * values, axis=-1, keepdims=True)
    return values * lax.rsqrt(mean_square + EPSILON) * gain_row.astype(jnp.float32)


def rotate(values, positions):
    half_dim = values.shape[-1] // 2
    frequency = jnp.power(
        ROPE_BASE, -2.0 * jnp.arange(half_dim, dtype=jnp.float32) / values.shape[-1]
    )
    angles = positions.astype(jnp.float32)[:, None] * frequency[None, :]
    cosine = jnp.cos(angles)[:, None, :]
    sine_table = jnp.sin(angles)[:, None, :]
    front_half = values[..., :half_dim]
    back_half = values[..., half_dim:]
    return jnp.concatenate(
        (
            front_half * cosine - back_half * sine_table,
            back_half * cosine + front_half * sine_table,
        ),
        axis=-1,
    )


def on_device(
    hidden,
    in_gain,
    post_gain,
    query_weight,
    key_weight,
    value_weight,
    out_weight,
    key_cache,
    value_cache,
    lengths,
    windowed,
):
    row_count = hidden.shape[0]
    query_width = query_weight.shape[2]
    key_width = key_weight.shape[2]
    seq_block = key_cache.shape[2]
    head_width = out_weight.shape[1]
    group_size = HEADS // KV_HEADS
    window_len = seq_block * lax.axis_size("mp") // 2
    keys_out = []
    values_out = []
    for layer_index in range(LAYERS):
        normed = rms_scale(hidden, in_gain[layer_index]).astype(jnp.bfloat16)
        token_slab = lax.all_to_all(normed, "dp", split_axis=1, concat_axis=0, tiled=True)
        joined = jnp.concatenate(
            (query_weight[layer_index], key_weight[layer_index], value_weight[layer_index]), 1
        )

        def local_term():
            part_rows = lax.slice_in_dim(token_slab, 0, row_count * lax.axis_size("dp"), axis=0)
            return jnp.dot(part_rows, joined, preferred_element_type=jnp.float32)

        summed = lax.psum_scatter(local_term(), "dp", scatter_dimension=0, tiled=True)
        query_part = summed[:, :query_width]
        key_part = summed[:, query_width : query_width + key_width]
        value_part = summed[:, query_width + key_width :]
        rounded = (
            query_part.astype(jnp.bfloat16),
            key_part.astype(jnp.bfloat16),
            value_part.astype(jnp.bfloat16),
        )
        query, key_raw, value_new = (
            lax.all_gather(rounded[0], "mp", axis=1, tiled=True),
            lax.all_gather(rounded[1], "mp", axis=1, tiled=True),
            lax.all_gather(rounded[2], "mp", axis=1, tiled=True),
        )
        queries = rotate(query.astype(jnp.float32).reshape(row_count, HEADS, HEAD_DIM), lengths)
        queries = (queries * HEAD_DIM ** (-0.5)).astype(jnp.bfloat16)
        keys_new = rotate(
            key_raw.astype(jnp.float32).reshape(row_count, KV_HEADS, HEAD_DIM), lengths
        ).astype(jnp.bfloat16)
        value_new = value_new.reshape(row_count, KV_HEADS, HEAD_DIM)
        grouped = queries.reshape(row_count, KV_HEADS, group_size, HEAD_DIM)
        scores = jnp.einsum(
            "rkgd,rskd->rkgs", grouped, key_cache[layer_index], preferred_element_type=jnp.float32
        )
        scores = SOFTCAP * jnp.tanh(scores / SOFTCAP)
        positions = lax.axis_index("mp") * seq_block + jnp.arange(seq_block, dtype=jnp.int32)
        window_flag = windowed[layer_index][:, None]
        usable = (positions[None, :] < lengths[:, None]) & (
            (window_flag == 0) | (positions[None, :] > lengths[:, None] - window_len)
        )
        usable = usable[:, None, None, :]
        masked = jnp.where(usable, scores, NEGATIVE)
        peaks = jnp.max(masked, axis=-1)
        exp_scores = jnp.where(usable, jnp.exp(masked - peaks[..., None]), 0.0)
        sums_exp = jnp.sum(exp_scores, axis=-1)
        accumulated = jnp.einsum(
            "rkgs,rskd->rkgd",
            exp_scores,
            value_cache[layer_index].astype(jnp.float32),
            preferred_element_type=jnp.float32,
        )
        global_peak = lax.pmax(peaks, "mp")
        rescale = jnp.exp(peaks - global_peak)
        sums_exp, accumulated = lax.psum(
            (sums_exp * rescale, accumulated * rescale[..., None]), "mp"
        )
        peaks = global_peak
        self_score = jnp.einsum(
            "rkgd,rkd->rkg", grouped, keys_new, preferred_element_type=jnp.float32
        )
        self_score = SOFTCAP * jnp.tanh(self_score / SOFTCAP)
        peak_all = jnp.maximum(peaks, self_score)
        old_scale = jnp.exp(peaks - peak_all)
        self_weight = jnp.exp(self_score - peak_all)
        denominator = sums_exp * old_scale + self_weight
        mixed = (
            accumulated * old_scale[..., None]
            + self_weight[..., None] * value_new.astype(jnp.float32)[:, :, None, :]
        )
        attended = (
            (mixed / denominator[..., None])
            .reshape(row_count, HEADS * HEAD_DIM)
            .astype(jnp.bfloat16)
        )
        attended_local = lax.dynamic_slice_in_dim(
            attended, lax.axis_index("mp") * head_width, head_width, 1
        )
        all_rows = lax.all_gather(attended_local, "dp", axis=0, tiled=True)
        partial_cols = jnp.dot(
            all_rows, out_weight[layer_index], preferred_element_type=jnp.float32
        )
        partial_cols = lax.psum(partial_cols, "mp")
        projected = lax.all_to_all(partial_cols, "dp", split_axis=0, concat_axis=1, tiled=True)
        hidden = (hidden.astype(jnp.float32) + rms_scale(projected, post_gain[layer_index])).astype(
            jnp.bfloat16
        )
        keys_out.append(keys_new)
        values_out.append(value_new)
    return (hidden, jnp.stack(keys_out), jnp.stack(values_out))


MESH_ID = pl.DeviceIdType.MESH
TILE_ROWS = 8


def fits(rows, dp, mp):
    return (
        mp & (mp - 1) == 0
        and dp & (dp - 1) == 0
        and HEADS % mp == 0
        and KV_HEADS % mp == 0
        and HEADS == 2 * KV_HEADS
        and rows * HEADS // mp == TILE_ROWS
    )


def low(index, size):
    return index & (size - 1)


def high(index, size):
    return index >> (size.bit_length() - 1)


def one_hot(rows, columns, match):
    row = lax.broadcasted_iota(jnp.int32, (rows, columns), 0)
    column = lax.broadcasted_iota(jnp.int32, (rows, columns), 1)
    return jnp.where(match(row, column), 1.0, 0.0).astype(jnp.bfloat16)


def partners(mine, count):
    found = []
    for pattern in range(count):
        there = 0
        for bit in range(count.bit_length() - 1):
            held = lax.rem(mine // 2**bit, 2)
            there = there + 2**bit * (1 - held if pattern >> bit & 1 else held)
        found.append(there)
    return found


def pick(selector, values):
    return jnp.dot(selector, values, preferred_element_type=jnp.float32)


def fused_kernel(
    dp,
    mp,
    lengths_hbm,
    windowed_hbm,
    hidden_hbm,
    in_gain_hbm,
    post_gain_hbm,
    query_hbm,
    key_hbm,
    value_hbm,
    out_hbm,
    key_cache_hbm,
    value_cache_hbm,
    hidden_out_ref,
    new_keys_ref,
    new_values_ref,
    lengths_ref,
    windowed_ref,
    hidden_ref,
    in_gain_ref,
    post_gain_ref,
    query_w,
    key_w,
    value_w,
    out_w,
    keys,
    values,
    norm_send,
    norm_recv,
    query_send,
    query_recv,
    pair_send,
    pair_recv,
    mix_send,
    mix_recv,
    sums_send,
    sums_recv,
    token_send,
    token_recv,
    cols_send,
    cols_recv,
    load_sem,
    send_sem,
    recv_sem,
):
    my_dp = lax.axis_index("dp")
    my_mp = lax.axis_index("mp")
    devices = dp * mp
    me = my_dp * mp + my_mp
    rows = hidden_ref.shape[0]
    total_rows = rows * dp
    slab = norm_send.shape[2]
    query_width = query_w.shape[1]
    key_width = key_w.shape[1]
    query_heads = query_width // HEAD_DIM
    key_heads = key_width // HEAD_DIM
    cache_rows = key_cache_hbm.shape[2]
    seq_block = cache_rows // KV_HEADS
    window_len = seq_block * mp // 2

    loads = [
        pltpu.make_async_copy(src, dst, load_sem.at[i])
        for i, (src, dst) in enumerate(
            (
                (hidden_hbm, hidden_ref),
                (in_gain_hbm, in_gain_ref),
                (lengths_hbm, lengths_ref),
                (windowed_hbm, windowed_ref),
                (query_hbm.at[0], query_w),
                (key_hbm.at[0], key_w),
                (value_hbm.at[0], value_w),
                (key_cache_hbm.at[0], keys),
                (value_cache_hbm.at[0], values),
                (out_hbm.at[0], out_w),
                (post_gain_hbm, post_gain_ref),
            )
        )
    ]
    peer_dp = partners(my_dp, dp)
    peer_mp = partners(my_mp, mp)
    others = [(i, j) for i in reversed(range(dp)) for j in reversed(range(mp)) if i + j > 0]
    barrier = pltpu.get_barrier_semaphore()
    for i, j in others:
        pl.semaphore_signal(
            barrier,
            inc=1,
            device_id={"dp": peer_dp[i], "mp": peer_mp[j]},
            device_id_type=MESH_ID,
        )
    for load in loads:
        load.start()
    for load in loads[:2]:
        load.wait()

    hidden = hidden_ref[...].astype(jnp.float32)
    mean_square = jnp.mean(hidden * hidden, axis=-1, keepdims=True)
    normed = hidden * lax.rsqrt(mean_square + EPSILON) * in_gain_ref[...]
    for part in range(dp):
        norm_send[part] = normed[:, part * slab : (part + 1) * slab].astype(jnp.bfloat16)

    pl.semaphore_wait(barrier, devices - 1)
    def finish(buffer, count, sem):
        block = buffer.at[pl.ds(0, count)]
        pltpu.make_async_copy(block, block, sem).wait()

    def exchange(recv, stage, targets, source, slot):
        for i, j in targets:
            pltpu.make_async_remote_copy(
                src_ref=source(peer_dp[i], peer_mp[j]),
                dst_ref=recv.at[slot],
                send_sem=send_sem.at[stage],
                recv_sem=recv_sem.at[stage],
                device_id={"dp": peer_dp[i], "mp": peer_mp[j]},
                device_id_type=MESH_ID,
            ).start()

    along_dp = [(i, j) for i, j in others if j == 0]
    along_mp = [(i, j) for i, j in others if i == 0]
    exchange(norm_recv, 0, along_dp, lambda a, b: norm_send.at[a], my_dp)
    norm_recv[my_dp] = norm_send[my_dp]
    for load in loads[2:4]:
        load.wait()

    block = rows * query_heads
    half = HEAD_DIM // 2
    lane = lax.broadcasted_iota(jnp.int32, (block, HEAD_DIM), 1)
    request = high(lax.broadcasted_iota(jnp.int32, (block, HEAD_DIM), 0), query_heads)
    pair = low(lane, half).astype(jnp.float32)
    frequency = jnp.exp(pair * (-2.0 / HEAD_DIM * math.log(ROPE_BASE)))
    place = jnp.full((block, HEAD_DIM), lengths_ref[0], jnp.int32)
    for r in range(1, rows):
        place = jnp.where(request == r, lengths_ref[r], place)
    angle = place.astype(jnp.float32) * frequency
    cosine = jnp.cos(angle)
    sine = jnp.sin(angle)
    sine = jnp.where(lane < half, -sine, sine)

    for load in loads[4:7]:
        load.wait()
    finish(norm_recv, dp - 1, recv_sem.at[0])
    tokens = jnp.concatenate(
        [norm_recv[part].astype(jnp.float32) for part in range(dp)], axis=0
    ).astype(jnp.bfloat16)
    spread = one_hot(
        total_rows * query_heads,
        total_rows * query_heads,
        lambda row, column: column
        == low(row, query_heads) * total_rows + high(row, query_heads),
    )

    def by_owner(parts):
        pieces = [
            part[:, at : at + HEAD_DIM]
            for part in parts
            for at in range(0, part.shape[1], HEAD_DIM)
        ]
        stacked = jnp.concatenate(pieces, axis=0).astype(jnp.bfloat16)
        return pick(spread, stacked).astype(jnp.bfloat16).reshape(dp, block, HEAD_DIM)

    query_send[...] = by_owner([pick(tokens, query_w[...])])
    exchange(query_recv, 1, others, lambda a, b: query_send.at[a], me)
    query_recv[me] = query_send[my_dp]
    pair_send[...] = by_owner([pick(tokens, key_w[...]), pick(tokens, value_w[...])])
    exchange(pair_recv, 2, along_dp, lambda a, b: pair_send.at[a], my_dp)
    pair_recv[my_dp] = pair_send[my_dp]

    for load in loads[7:9]:
        load.wait()
    group_rows = mp * block
    row = lax.broadcasted_iota(jnp.int32, (group_rows, cache_rows), 0)
    column = lax.broadcasted_iota(jnp.int32, (group_rows, cache_rows), 1)
    head_match = low(column, KV_HEADS) == high(row, block) * key_heads + high(
        low(row, query_heads), 2
    )
    row_request = high(low(row, block), query_heads)
    position = my_mp * seq_block + high(column, KV_HEADS)
    allowed = []
    for r in range(rows):
        length = lengths_ref[r]
        floor = jnp.where(windowed_ref[0, r] == 0, -1, length - window_len)
        allowed.append(
            head_match & (row_request == r) & (position < length) & (position > floor)
        )
    own_row = lax.broadcasted_iota(jnp.int32, (group_rows, block), 0)
    own_column = lax.broadcasted_iota(jnp.int32, (group_rows, block), 1)
    own_base = low(own_row, block) - low(own_row, query_heads) + high(low(own_row, query_heads), 2)
    own_group = high(own_row, block) == my_mp
    own_key = own_group & (own_column == own_base)
    own_value = jnp.where(own_column == own_base + key_heads, 1.0, 0.0).astype(jnp.bfloat16)
    group_lane = lax.broadcasted_iota(jnp.int32, (group_rows, HEAD_DIM), 1)
    group_row = low(lax.broadcasted_iota(jnp.int32, (group_rows, HEAD_DIM), 0), block)
    over_last = (((1,), (1,)), ((), ()))

    def turn(raw):
        return raw * cosine + pltpu.roll(raw, half, raw.ndim - 1) * sine

    finish(query_recv, devices - 1, recv_sem.at[1])
    raw = jnp.sum(
        query_recv[...].astype(jnp.float32).reshape(dp, mp, block, HEAD_DIM), axis=0
    )
    raw = raw.astype(jnp.bfloat16).astype(jnp.float32)
    queries = jnp.concatenate([turn(raw[m]) for m in range(mp)], axis=0)
    queries = (queries * HEAD_DIM ** (-0.5)).astype(jnp.bfloat16)
    accumulated = jnp.zeros((group_rows, HEAD_DIM), jnp.float32)
    sums_exp = jnp.zeros((group_rows, 1), jnp.float32)
    for r in range(rows):
        scores = lax.dot_general(
            queries, keys[r], over_last, preferred_element_type=jnp.float32
        )
        scores = SOFTCAP * jnp.tanh(scores * (1.0 / SOFTCAP))
        exp_scores = jnp.where(allowed[r], jnp.exp(scores), 0.0)
        sums_exp = sums_exp + jnp.sum(exp_scores, axis=-1, keepdims=True)
        accumulated = accumulated + pick(exp_scores.astype(jnp.bfloat16), values[r])

    finish(pair_recv, dp - 1, recv_sem.at[2])
    pair_raw = jnp.sum(pair_recv[...].astype(jnp.float32), axis=0).astype(jnp.bfloat16)
    pair_wide = pair_raw.astype(jnp.float32)
    token = turn(pair_wide).astype(jnp.bfloat16)
    own = lax.dot_general(queries, token, over_last, preferred_element_type=jnp.float32)
    own = jnp.sum(jnp.where(own_key, own, 0.0), axis=-1, keepdims=True)
    own = jnp.exp(SOFTCAP * jnp.tanh(own * (1.0 / SOFTCAP)))
    own = jnp.where(own_group[:, :1], own, 0.0)
    accumulated = accumulated + own * pick(own_value, pair_raw)
    sums_exp = sums_exp + own
    mix_send[...] = accumulated.reshape(mp, block, HEAD_DIM).astype(mix_send.dtype)
    sums_send[...] = jnp.sum(
        jnp.where(group_lane == group_row, sums_exp, 0.0).reshape(mp, block, HEAD_DIM),
        axis=1,
        keepdims=True,
    )
    exchange(mix_recv, 3, others, lambda a, b: mix_send.at[b], me)
    exchange(sums_recv, 4, others, lambda a, b: sums_send.at[b], me)
    mix_recv[me] = mix_send[my_mp]
    sums_recv[me] = sums_send[my_mp]
    is_key = low(lax.broadcasted_iota(jnp.int32, (block, HEAD_DIM), 0), query_heads) < key_heads
    token_send[...] = jnp.where(is_key, token.astype(jnp.float32), pair_wide).astype(jnp.bfloat16)
    exchange(token_recv, 5, along_mp, lambda a, b: token_send, my_mp)
    token_recv[my_mp] = token_send[...]

    gather = one_hot(
        query_heads * total_rows,
        query_heads * total_rows,
        lambda row, column: column
        == low(row, total_rows) * query_heads + high(row, total_rows),
    )
    for load in loads[9:]:
        load.wait()
    finish(mix_recv, devices - 1, recv_sem.at[3])
    mixed = jnp.sum(
        mix_recv[...].astype(jnp.float32).reshape(dp, mp, block, HEAD_DIM), axis=1
    )
    finish(sums_recv, devices - 1, recv_sem.at[4])
    sums = jnp.sum(sums_recv[...].reshape(dp, mp, 1, HEAD_DIM), axis=1)
    at_row = lax.broadcasted_iota(jnp.int32, mixed.shape, 1)
    at_lane = lax.broadcasted_iota(jnp.int32, mixed.shape, 2)
    sums = jnp.sum(jnp.where(at_row == at_lane, sums, 0.0), axis=-1, keepdims=True)
    attended = (mixed / sums).reshape(dp * block, HEAD_DIM).astype(jnp.bfloat16)
    heads = pick(gather, attended).astype(jnp.bfloat16)
    heads = jnp.concatenate(
        [heads[b * total_rows : (b + 1) * total_rows] for b in range(query_heads)], axis=1
    )
    partial_cols = lax.dot_general(
        heads, out_w[...], over_last, preferred_element_type=jnp.float32
    )
    for part in range(dp):
        cols_send[part] = partial_cols[part * rows : (part + 1) * rows].astype(cols_send.dtype)
    exchange(cols_recv, 6, others, lambda a, b: cols_send.at[a], me)
    cols_recv[me] = cols_send[my_dp]

    def owner(row, first):
        head = low(row, KV_HEADS)
        return (
            high(head, key_heads) * block
            + high(row, KV_HEADS) * query_heads
            + first
            + low(head, key_heads)
        )

    finish(token_recv, mp - 1, recv_sem.at[5])
    tokens_new = token_recv[...].astype(jnp.float32).reshape(group_rows, HEAD_DIM)
    tokens_new = tokens_new.astype(jnp.bfloat16)
    for first, out_ref in ((0, new_keys_ref), (key_heads, new_values_ref)):
        chosen = one_hot(
            rows * KV_HEADS, group_rows, lambda row, column: column == owner(row, first)
        )
        out_ref[...] = pick(chosen, tokens_new).astype(jnp.bfloat16).reshape(out_ref.shape)
    finish(cols_recv, devices - 1, recv_sem.at[6])
    pieces = []
    for part in range(dp):
        piece = cols_recv[part * mp].astype(jnp.float32)
        for other in range(1, mp):
            piece = piece + cols_recv[part * mp + other].astype(jnp.float32)
        pieces.append(piece)
    projected = jnp.concatenate(pieces, axis=1)
    mean_square = jnp.mean(projected * projected, axis=-1, keepdims=True)
    update = projected * lax.rsqrt(mean_square + EPSILON) * post_gain_ref[...]
    hidden_out_ref[...] = (hidden_ref[...].astype(jnp.float32) + update).astype(jnp.bfloat16)

    finish(norm_recv, dp - 1, send_sem.at[0])
    finish(query_recv, devices - 1, send_sem.at[1])
    finish(pair_recv, dp - 1, send_sem.at[2])
    finish(mix_recv, devices - 1, send_sem.at[3])
    finish(sums_recv, devices - 1, send_sem.at[4])
    finish(token_recv, mp - 1, send_sem.at[5])
    finish(cols_recv, devices - 1, send_sem.at[6])


def copy_kernel(a_ref, b_ref, c_ref, a_out, b_out, c_out):
    a_out[...] = a_ref[...]
    b_out[...] = b_ref[...]
    c_out[...] = c_ref[...]


def fused_device(
    hidden,
    in_gain,
    post_gain,
    query_weight,
    key_weight,
    value_weight,
    out_weight,
    key_cache,
    value_cache,
    lengths,
    windowed,
):
    dp = lax.axis_size("dp")
    mp = lax.axis_size("mp")
    rows = hidden.shape[0]
    slab = query_weight.shape[1]
    out_slab = out_weight.shape[2]
    block = rows * query_weight.shape[2] // HEAD_DIM
    half_word = jnp.bfloat16
    flat = (LAYERS, rows, key_cache.shape[2] * KV_HEADS, HEAD_DIM)
    out_shape = (
        jax.ShapeDtypeStruct(hidden.shape, half_word),
        jax.ShapeDtypeStruct((LAYERS, rows, KV_HEADS, HEAD_DIM), half_word),
        jax.ShapeDtypeStruct((LAYERS, rows, KV_HEADS, HEAD_DIM), half_word),
    )
    vmem = pl.BlockSpec(memory_space=pltpu.VMEM)
    far = pl.BlockSpec(memory_space=pl.ANY)
    results = pl.pallas_call(
        functools.partial(fused_kernel, dp, mp),
        out_shape=out_shape,
        in_specs=[far] * 11,
        out_specs=(vmem, vmem, vmem),
        scratch_shapes=[
            pltpu.SMEM(lengths.shape, lengths.dtype),
            pltpu.SMEM(windowed.shape, windowed.dtype),
            pltpu.VMEM(hidden.shape, hidden.dtype),
            pltpu.VMEM(in_gain.shape, in_gain.dtype),
            pltpu.VMEM(post_gain.shape, post_gain.dtype),
            pltpu.VMEM(query_weight.shape[1:], half_word),
            pltpu.VMEM(key_weight.shape[1:], half_word),
            pltpu.VMEM(value_weight.shape[1:], half_word),
            pltpu.VMEM((out_slab, out_weight.shape[1]), half_word),
            pltpu.VMEM(flat[1:], half_word),
            pltpu.VMEM(flat[1:], half_word),
            pltpu.VMEM((dp, rows, slab), half_word),
            pltpu.VMEM((dp, rows, slab), half_word),
            pltpu.VMEM((dp, block, HEAD_DIM), half_word),
            pltpu.VMEM((dp * mp, block, HEAD_DIM), half_word),
            pltpu.VMEM((dp, block, HEAD_DIM), half_word),
            pltpu.VMEM((dp, block, HEAD_DIM), half_word),
            pltpu.VMEM((mp, block, HEAD_DIM), half_word),
            pltpu.VMEM((dp * mp, block, HEAD_DIM), half_word),
            pltpu.VMEM((mp, 1, HEAD_DIM), jnp.float32),
            pltpu.VMEM((dp * mp, 1, HEAD_DIM), jnp.float32),
            pltpu.VMEM((block, HEAD_DIM), half_word),
            pltpu.VMEM((mp, block, HEAD_DIM), half_word),
            pltpu.VMEM((dp, rows, out_slab), half_word),
            pltpu.VMEM((dp * mp, rows, out_slab), half_word),
            pltpu.SemaphoreType.DMA((11,)),
            pltpu.SemaphoreType.DMA((7,)),
            pltpu.SemaphoreType.DMA((7,)),
        ],
        compiler_params=pltpu.CompilerParams(collective_id=0, has_side_effects=True),
    )(
        lengths,
        windowed,
        hidden,
        in_gain,
        post_gain,
        query_weight,
        key_weight,
        value_weight,
        jnp.swapaxes(out_weight, 1, 2),
        key_cache.reshape(flat),
        value_cache.reshape(flat),
    )
    plain = pl.pallas_call(copy_kernel, out_shape=out_shape, in_specs=[vmem] * 3, out_specs=(vmem,) * 3)
    return plain(*results)


def device_step(hidden, *rest):
    fused = fits(hidden.shape[0], lax.axis_size("dp"), lax.axis_size("mp"))
    return (fused_device if fused else on_device)(hidden, *rest)


def solution(mesh):
    return jax.shard_map(
        device_step,
        mesh=mesh,
        in_specs=(
            P("dp", None),
            P(),
            P(),
            P(None, "dp", "mp"),
            P(None, "dp", "mp"),
            P(None, "dp", "mp"),
            P(None, "mp", "dp"),
            P(None, "dp", "mp", None, None),
            P(None, "dp", "mp", None, None),
            P("dp"),
            P(None, "dp"),
        ),
        out_specs=(P("dp", None), P(None, "dp", None, None), P(None, "dp", None, None)),
        check_vma=False,
    )
```

```python
import functools
import math

import jax
import jax.numpy as jnp
from jax import lax
from jax.experimental import pallas as pl
from jax.experimental.pallas import tpu as pltpu
from jax.sharding import PartitionSpec as P

HEADS = 16
KV_HEADS = 8
HEAD_DIM = 128
LAYERS = 1


EPSILON = 1e-06
SOFTCAP = 50.0
ROPE_BASE = 10000.0
NEGATIVE = -1e30


def rms_scale(values, gain_row):
    values = values.astype(jnp.float32)
    mean_square = jnp.mean(values * values, axis=-1, keepdims=True)
    return values * lax.rsqrt(mean_square + EPSILON) * gain_row.astype(jnp.float32)


def rotate(values, positions):
    half_dim = values.shape[-1] // 2
    frequency = jnp.power(
        ROPE_BASE, -2.0 * jnp.arange(half_dim, dtype=jnp.float32) / values.shape[-1]
    )
    angles = positions.astype(jnp.float32)[:, None] * frequency[None, :]
    cosine = jnp.cos(angles)[:, None, :]
    sine_table = jnp.sin(angles)[:, None, :]
    front_half = values[..., :half_dim]
    back_half = values[..., half_dim:]
    return jnp.concatenate(
        (
            front_half * cosine - back_half * sine_table,
            back_half * cosine + front_half * sine_table,
        ),
        axis=-1,
    )


def on_device(
    hidden,
    in_gain,
    post_gain,
    query_weight,
    key_weight,
    value_weight,
    out_weight,
    key_cache,
    value_cache,
    lengths,
    windowed,
):
    row_count = hidden.shape[0]
    query_width = query_weight.shape[2]
    key_width = key_weight.shape[2]
    seq_block = key_cache.shape[2]
    head_width = out_weight.shape[1]
    group_size = HEADS // KV_HEADS
    window_len = seq_block * lax.axis_size("mp") // 2
    keys_out = []
    values_out = []
    for layer_index in range(LAYERS):
        normed = rms_scale(hidden, in_gain[layer_index]).astype(jnp.bfloat16)
        token_slab = lax.all_to_all(normed, "dp", split_axis=1, concat_axis=0, tiled=True)
        joined = jnp.concatenate(
            (query_weight[layer_index], key_weight[layer_index], value_weight[layer_index]), 1
        )

        def local_term():
            part_rows = lax.slice_in_dim(token_slab, 0, row_count * lax.axis_size("dp"), axis=0)
            return jnp.dot(part_rows, joined, preferred_element_type=jnp.float32)

        summed = lax.psum_scatter(local_term(), "dp", scatter_dimension=0, tiled=True)
        query_part = summed[:, :query_width]
        key_part = summed[:, query_width : query_width + key_width]
        value_part = summed[:, query_width + key_width :]
        rounded = (
            query_part.astype(jnp.bfloat16),
            key_part.astype(jnp.bfloat16),
            value_part.astype(jnp.bfloat16),
        )
        query, key_raw, value_new = (
            lax.all_gather(rounded[0], "mp", axis=1, tiled=True),
            lax.all_gather(rounded[1], "mp", axis=1, tiled=True),
            lax.all_gather(rounded[2], "mp", axis=1, tiled=True),
        )
        queries = rotate(query.astype(jnp.float32).reshape(row_count, HEADS, HEAD_DIM), lengths)
        queries = (queries * HEAD_DIM ** (-0.5)).astype(jnp.bfloat16)
        keys_new = rotate(
            key_raw.astype(jnp.float32).reshape(row_count, KV_HEADS, HEAD_DIM), lengths
        ).astype(jnp.bfloat16)
        value_new = value_new.reshape(row_count, KV_HEADS, HEAD_DIM)
        grouped = queries.reshape(row_count, KV_HEADS, group_size, HEAD_DIM)
        scores = jnp.einsum(
            "rkgd,rskd->rkgs", grouped, key_cache[layer_index], preferred_element_type=jnp.float32
        )
        scores = SOFTCAP * jnp.tanh(scores / SOFTCAP)
        positions = lax.axis_index("mp") * seq_block + jnp.arange(seq_block, dtype=jnp.int32)
        window_flag = windowed[layer_index][:, None]
        usable = (positions[None, :] < lengths[:, None]) & (
            (window_flag == 0) | (positions[None, :] > lengths[:, None] - window_len)
        )
        usable = usable[:, None, None, :]
        masked = jnp.where(usable, scores, NEGATIVE)
        peaks = jnp.max(masked, axis=-1)
        exp_scores = jnp.where(usable, jnp.exp(masked - peaks[..., None]), 0.0)
        sums_exp = jnp.sum(exp_scores, axis=-1)
        accumulated = jnp.einsum(
            "rkgs,rskd->rkgd",
            exp_scores,
            value_cache[layer_index].astype(jnp.float32),
            preferred_element_type=jnp.float32,
        )
        global_peak = lax.pmax(peaks, "mp")
        rescale = jnp.exp(peaks - global_peak)
        sums_exp, accumulated = lax.psum(
            (sums_exp * rescale, accumulated * rescale[..., None]), "mp"
        )
        peaks = global_peak
        self_score = jnp.einsum(
            "rkgd,rkd->rkg", grouped, keys_new, preferred_element_type=jnp.float32
        )
        self_score = SOFTCAP * jnp.tanh(self_score / SOFTCAP)
        peak_all = jnp.maximum(peaks, self_score)
        old_scale = jnp.exp(peaks - peak_all)
        self_weight = jnp.exp(self_score - peak_all)
        denominator = sums_exp * old_scale + self_weight
        mixed = (
            accumulated * old_scale[..., None]
            + self_weight[..., None] * value_new.astype(jnp.float32)[:, :, None, :]
        )
        attended = (
            (mixed / denominator[..., None])
            .reshape(row_count, HEADS * HEAD_DIM)
            .astype(jnp.bfloat16)
        )
        attended_local = lax.dynamic_slice_in_dim(
            attended, lax.axis_index("mp") * head_width, head_width, 1
        )
        all_rows = lax.all_gather(attended_local, "dp", axis=0, tiled=True)
        partial_cols = jnp.dot(
            all_rows, out_weight[layer_index], preferred_element_type=jnp.float32
        )
        partial_cols = lax.psum(partial_cols, "mp")
        projected = lax.all_to_all(partial_cols, "dp", split_axis=0, concat_axis=1, tiled=True)
        hidden = (hidden.astype(jnp.float32) + rms_scale(projected, post_gain[layer_index])).astype(
            jnp.bfloat16
        )
        keys_out.append(keys_new)
        values_out.append(value_new)
    return (hidden, jnp.stack(keys_out), jnp.stack(values_out))


MESH_ID = pl.DeviceIdType.MESH
TILE_ROWS = 8


def fits(rows, dp, mp):
    return (
        mp & (mp - 1) == 0
        and dp & (dp - 1) == 0
        and HEADS % mp == 0
        and KV_HEADS % mp == 0
        and HEADS == 2 * KV_HEADS
        and rows * HEADS // mp == TILE_ROWS
    )


def low(index, size):
    return index & (size - 1)


def high(index, size):
    return index >> (size.bit_length() - 1)


def one_hot(rows, columns, match):
    row = lax.broadcasted_iota(jnp.int32, (rows, columns), 0)
    column = lax.broadcasted_iota(jnp.int32, (rows, columns), 1)
    return jnp.where(match(row, column), 1.0, 0.0).astype(jnp.bfloat16)


def partners(mine, count):
    found = []
    for pattern in range(count):
        there = 0
        for bit in range(count.bit_length() - 1):
            held = lax.rem(mine // 2**bit, 2)
            there = there + 2**bit * (1 - held if pattern >> bit & 1 else held)
        found.append(there)
    return found


def pick(selector, values):
    return jnp.dot(selector, values, preferred_element_type=jnp.float32)


def fused_kernel(
    dp,
    mp,
    lengths_hbm,
    windowed_hbm,
    hidden_hbm,
    in_gain_hbm,
    post_gain_hbm,
    query_hbm,
    key_hbm,
    value_hbm,
    out_hbm,
    key_cache_hbm,
    value_cache_hbm,
    hidden_out_ref,
    new_keys_ref,
    new_values_ref,
    lengths_ref,
    windowed_ref,
    hidden_ref,
    in_gain_ref,
    post_gain_ref,
    query_w,
    key_w,
    value_w,
    out_w,
    keys,
    values,
    norm_send,
    norm_recv,
    query_send,
    query_recv,
    pair_send,
    pair_recv,
    mix_send,
    mix_recv,
    sums_send,
    sums_recv,
    token_send,
    token_recv,
    cols_send,
    cols_recv,
    load_sem,
    send_sem,
    recv_sem,
):
    my_dp = lax.axis_index("dp")
    my_mp = lax.axis_index("mp")
    devices = dp * mp
    me = my_dp * mp + my_mp
    rows = hidden_ref.shape[0]
    total_rows = rows * dp
    slab = norm_send.shape[2]
    query_width = query_w.shape[1]
    key_width = key_w.shape[1]
    query_heads = query_width // HEAD_DIM
    key_heads = key_width // HEAD_DIM
    cache_rows = key_cache_hbm.shape[2]
    seq_block = cache_rows // KV_HEADS
    window_len = seq_block * mp // 2

    loads = [
        pltpu.make_async_copy(src, dst, load_sem.at[i])
        for i, (src, dst) in enumerate(
            (
                (hidden_hbm, hidden_ref),
                (in_gain_hbm, in_gain_ref),
                (lengths_hbm, lengths_ref),
                (windowed_hbm, windowed_ref),
                (query_hbm.at[0], query_w),
                (key_hbm.at[0], key_w),
                (value_hbm.at[0], value_w),
                (key_cache_hbm.at[0], keys),
                (value_cache_hbm.at[0], values),
                (out_hbm.at[0], out_w),
                (post_gain_hbm, post_gain_ref),
            )
        )
    ]
    peer_dp = partners(my_dp, dp)
    peer_mp = partners(my_mp, mp)
    others = [(i, j) for i in reversed(range(dp)) for j in reversed(range(mp)) if i + j > 0]
    barrier = pltpu.get_barrier_semaphore()
    for i, j in others:
        pl.semaphore_signal(
            barrier,
            inc=1,
            device_id={"dp": peer_dp[i], "mp": peer_mp[j]},
            device_id_type=MESH_ID,
        )
    for load in loads:
        load.start()
    for load in loads[:2]:
        load.wait()

    hidden = hidden_ref[...].astype(jnp.float32)
    mean_square = jnp.mean(hidden * hidden, axis=-1, keepdims=True)
    normed = hidden * lax.rsqrt(mean_square + EPSILON) * in_gain_ref[...]
    for part in range(dp):
        norm_send[part] = normed[:, part * slab : (part + 1) * slab].astype(jnp.bfloat16)

    pl.semaphore_wait(barrier, devices - 1)
    def finish(buffer, count, sem):
        block = buffer.at[pl.ds(0, count)]
        pltpu.make_async_copy(block, block, sem).wait()

    def exchange(recv, stage, targets, source, slot):
        for i, j in targets:
            pltpu.make_async_remote_copy(
                src_ref=source(peer_dp[i], peer_mp[j]),
                dst_ref=recv.at[slot],
                send_sem=send_sem.at[stage],
                recv_sem=recv_sem.at[stage],
                device_id={"dp": peer_dp[i], "mp": peer_mp[j]},
                device_id_type=MESH_ID,
            ).start()

    along_dp = [(i, j) for i, j in others if j == 0]
    along_mp = [(i, j) for i, j in others if i == 0]
    exchange(norm_recv, 0, along_dp, lambda a, b: norm_send.at[a], my_dp)
    norm_recv[my_dp] = norm_send[my_dp]
    for load in loads[2:4]:
        load.wait()

    block = rows * query_heads
    half = HEAD_DIM // 2
    lane = lax.broadcasted_iota(jnp.int32, (block, HEAD_DIM), 1)
    request = high(lax.broadcasted_iota(jnp.int32, (block, HEAD_DIM), 0), query_heads)
    pair = low(lane, half).astype(jnp.float32)
    frequency = jnp.exp(pair * (-2.0 / HEAD_DIM * math.log(ROPE_BASE)))
    place = jnp.full((block, HEAD_DIM), lengths_ref[0], jnp.int32)
    for r in range(1, rows):
        place = jnp.where(request == r, lengths_ref[r], place)
    angle = place.astype(jnp.float32) * frequency
    cosine = jnp.cos(angle)
    sine = jnp.sin(angle)
    sine = jnp.where(lane < half, -sine, sine)

    for load in loads[4:7]:
        load.wait()
    finish(norm_recv, dp - 1, recv_sem.at[0])
    tokens = jnp.concatenate(
        [norm_recv[part].astype(jnp.float32) for part in range(dp)], axis=0
    ).astype(jnp.bfloat16)
    spread = one_hot(
        total_rows * query_heads,
        total_rows * query_heads,
        lambda row, column: column
        == low(row, query_heads) * total_rows + high(row, query_heads),
    )

    def by_owner(parts):
        pieces = [
            part[:, at : at + HEAD_DIM]
            for part in parts
            for at in range(0, part.shape[1], HEAD_DIM)
        ]
        stacked = jnp.concatenate(pieces, axis=0).astype(jnp.bfloat16)
        return pick(spread, stacked).astype(jnp.bfloat16).reshape(dp, block, HEAD_DIM)

    query_send[...] = by_owner([pick(tokens, query_w[...])])
    exchange(query_recv, 1, others, lambda a, b: query_send.at[a], me)
    query_recv[me] = query_send[my_dp]
    pair_send[...] = by_owner([pick(tokens, key_w[...]), pick(tokens, value_w[...])])
    exchange(pair_recv, 2, along_dp, lambda a, b: pair_send.at[a], my_dp)
    pair_recv[my_dp] = pair_send[my_dp]

    for load in loads[7:9]:
        load.wait()
    group_rows = mp * block
    row = lax.broadcasted_iota(jnp.int32, (group_rows, cache_rows), 0)
    column = lax.broadcasted_iota(jnp.int32, (group_rows, cache_rows), 1)
    head_match = low(column, KV_HEADS) == high(row, block) * key_heads + high(
        low(row, query_heads), 2
    )
    row_request = high(low(row, block), query_heads)
    position = my_mp * seq_block + high(column, KV_HEADS)
    allowed = []
    for r in range(rows):
        length = lengths_ref[r]
        floor = jnp.where(windowed_ref[0, r] == 0, -1, length - window_len)
        allowed.append(
            head_match & (row_request == r) & (position < length) & (position > floor)
        )
    own_row = lax.broadcasted_iota(jnp.int32, (group_rows, block), 0)
    own_column = lax.broadcasted_iota(jnp.int32, (group_rows, block), 1)
    own_base = low(own_row, block) - low(own_row, query_heads) + high(low(own_row, query_heads), 2)
    own_group = high(own_row, block) == my_mp
    own_key = own_group & (own_column == own_base)
    own_value = jnp.where(own_column == own_base + key_heads, 1.0, 0.0).astype(jnp.bfloat16)
    group_lane = lax.broadcasted_iota(jnp.int32, (group_rows, HEAD_DIM), 1)
    group_row = low(lax.broadcasted_iota(jnp.int32, (group_rows, HEAD_DIM), 0), block)
    over_last = (((1,), (1,)), ((), ()))

    def turn(raw):
        return raw * cosine + pltpu.roll(raw, half, raw.ndim - 1) * sine

    finish(query_recv, devices - 1, recv_sem.at[1])
    raw = jnp.sum(
        query_recv[...].astype(jnp.float32).reshape(dp, mp, block, HEAD_DIM), axis=0
    )
    raw = raw.astype(jnp.bfloat16).astype(jnp.float32)
    queries = jnp.concatenate([turn(raw[m]) for m in range(mp)], axis=0)
    queries = (queries * HEAD_DIM ** (-0.5)).astype(jnp.bfloat16)
    accumulated = jnp.zeros((group_rows, HEAD_DIM), jnp.float32)
    sums_exp = jnp.zeros((group_rows, 1), jnp.float32)
    for r in range(rows):
        scores = lax.dot_general(
            queries, keys[r], over_last, preferred_element_type=jnp.float32
        )
        scores = SOFTCAP * jnp.tanh(scores * (1.0 / SOFTCAP))
        exp_scores = jnp.where(allowed[r], jnp.exp(scores), 0.0)
        sums_exp = sums_exp + jnp.sum(exp_scores, axis=-1, keepdims=True)
        accumulated = accumulated + pick(exp_scores.astype(jnp.bfloat16), values[r])

    finish(pair_recv, dp - 1, recv_sem.at[2])
    pair_raw = jnp.sum(pair_recv[...].astype(jnp.float32), axis=0).astype(jnp.bfloat16)
    pair_wide = pair_raw.astype(jnp.float32)
    token = turn(pair_wide).astype(jnp.bfloat16)
    own = lax.dot_general(queries, token, over_last, preferred_element_type=jnp.float32)
    own = jnp.sum(jnp.where(own_key, own, 0.0), axis=-1, keepdims=True)
    own = jnp.exp(SOFTCAP * jnp.tanh(own * (1.0 / SOFTCAP)))
    own = jnp.where(own_group[:, :1], own, 0.0)
    accumulated = accumulated + own * pick(own_value, pair_raw)
    sums_exp = sums_exp + own
    mix_send[...] = accumulated.reshape(mp, block, HEAD_DIM).astype(mix_send.dtype)
    sums_send[...] = jnp.sum(
        jnp.where(group_lane == group_row, sums_exp, 0.0).reshape(mp, block, HEAD_DIM),
        axis=1,
        keepdims=True,
    )
    exchange(mix_recv, 3, others, lambda a, b: mix_send.at[b], me)
    exchange(sums_recv, 4, others, lambda a, b: sums_send.at[b], me)
    mix_recv[me] = mix_send[my_mp]
    sums_recv[me] = sums_send[my_mp]
    is_key = low(lax.broadcasted_iota(jnp.int32, (block, HEAD_DIM), 0), query_heads) < key_heads
    token_send[...] = jnp.where(is_key, token.astype(jnp.float32), pair_wide).astype(jnp.bfloat16)
    exchange(token_recv, 5, along_mp, lambda a, b: token_send, my_mp)
    token_recv[my_mp] = token_send[...]

    gather = one_hot(
        query_heads * total_rows,
        query_heads * total_rows,
        lambda row, column: column
        == low(row, total_rows) * query_heads + high(row, total_rows),
    )
    for load in loads[9:]:
        load.wait()
    finish(mix_recv, devices - 1, recv_sem.at[3])
    mixed = jnp.sum(
        mix_recv[...].astype(jnp.float32).reshape(dp, mp, block, HEAD_DIM), axis=1
    )
    finish(sums_recv, devices - 1, recv_sem.at[4])
    sums = jnp.sum(sums_recv[...].reshape(dp, mp, 1, HEAD_DIM), axis=1)
    at_row = lax.broadcasted_iota(jnp.int32, mixed.shape, 1)
    at_lane = lax.broadcasted_iota(jnp.int32, mixed.shape, 2)
    sums = jnp.sum(jnp.where(at_row == at_lane, sums, 0.0), axis=-1, keepdims=True)
    attended = (mixed / sums).reshape(dp * block, HEAD_DIM).astype(jnp.bfloat16)
    heads = pick(gather, attended).astype(jnp.bfloat16)
    heads = jnp.concatenate(
        [heads[b * total_rows : (b + 1) * total_rows] for b in range(query_heads)], axis=1
    )
    partial_cols = lax.dot_general(
        heads, out_w[...], over_last, preferred_element_type=jnp.float32
    )
    for part in range(dp):
        cols_send[part] = partial_cols[part * rows : (part + 1) * rows].astype(cols_send.dtype)
    exchange(cols_recv, 6, others, lambda a, b: cols_send.at[a], me)
    cols_recv[me] = cols_send[my_dp]

    def owner(row, first):
        head = low(row, KV_HEADS)
        return (
            high(head, key_heads) * block
            + high(row, KV_HEADS) * query_heads
            + first
            + low(head, key_heads)
        )

    finish(token_recv, mp - 1, recv_sem.at[5])
    tokens_new = token_recv[...].astype(jnp.float32).reshape(group_rows, HEAD_DIM)
    tokens_new = tokens_new.astype(jnp.bfloat16)
    for first, out_ref in ((0, new_keys_ref), (key_heads, new_values_ref)):
        chosen = one_hot(
            rows * KV_HEADS, group_rows, lambda row, column: column == owner(row, first)
        )
        out_ref[...] = pick(chosen, tokens_new).astype(jnp.bfloat16).reshape(out_ref.shape)
    finish(cols_recv, devices - 1, recv_sem.at[6])
    pieces = []
    for part in range(dp):
        piece = cols_recv[part * mp].astype(jnp.float32)
        for other in range(1, mp):
            piece = piece + cols_recv[part * mp + other].astype(jnp.float32)
        pieces.append(piece)
    projected = jnp.concatenate(pieces, axis=1)
    mean_square = jnp.mean(projected * projected, axis=-1, keepdims=True)
    update = projected * lax.rsqrt(mean_square + EPSILON) * post_gain_ref[...]
    hidden_out_ref[...] = (hidden_ref[...].astype(jnp.float32) + update).astype(jnp.bfloat16)

    finish(norm_recv, dp - 1, send_sem.at[0])
    finish(query_recv, devices - 1, send_sem.at[1])
    finish(pair_recv, dp - 1, send_sem.at[2])
    finish(mix_recv, devices - 1, send_sem.at[3])
    finish(sums_recv, devices - 1, send_sem.at[4])
    finish(token_recv, mp - 1, send_sem.at[5])
    finish(cols_recv, devices - 1, send_sem.at[6])


def copy_kernel(a_ref, b_ref, c_ref, a_out, b_out, c_out):
    a_out[...] = a_ref[...]
    b_out[...] = b_ref[...]
    c_out[...] = c_ref[...]


def fused_device(
    hidden,
    in_gain,
    post_gain,
    query_weight,
    key_weight,
    value_weight,
    out_weight,
    key_cache,
    value_cache,
    lengths,
    windowed,
):
    dp = lax.axis_size("dp")
    mp = lax.axis_size("mp")
    rows = hidden.shape[0]
    slab = query_weight.shape[1]
    out_slab = out_weight.shape[2]
    block = rows * query_weight.shape[2] // HEAD_DIM
    half_word = jnp.bfloat16
    flat = (LAYERS, rows, key_cache.shape[2] * KV_HEADS, HEAD_DIM)
    out_shape = (
        jax.ShapeDtypeStruct(hidden.shape, half_word),
        jax.ShapeDtypeStruct((LAYERS, rows, KV_HEADS, HEAD_DIM), half_word),
        jax.ShapeDtypeStruct((LAYERS, rows, KV_HEADS, HEAD_DIM), half_word),
    )
    vmem = pl.BlockSpec(memory_space=pltpu.VMEM)
    far = pl.BlockSpec(memory_space=pl.ANY)
    results = pl.pallas_call(
        functools.partial(fused_kernel, dp, mp),
        out_shape=tuple(pltpu.VMEM(held.shape, held.dtype) for held in out_shape),
        in_specs=[far] * 11,
        out_specs=(vmem, vmem, vmem),
        scratch_shapes=[
            pltpu.SMEM(lengths.shape, lengths.dtype),
            pltpu.SMEM(windowed.shape, windowed.dtype),
            pltpu.VMEM(hidden.shape, hidden.dtype),
            pltpu.VMEM(in_gain.shape, in_gain.dtype),
            pltpu.VMEM(post_gain.shape, post_gain.dtype),
            pltpu.VMEM(query_weight.shape[1:], half_word),
            pltpu.VMEM(key_weight.shape[1:], half_word),
            pltpu.VMEM(value_weight.shape[1:], half_word),
            pltpu.VMEM((out_slab, out_weight.shape[1]), half_word),
            pltpu.VMEM(flat[1:], half_word),
            pltpu.VMEM(flat[1:], half_word),
            pltpu.VMEM((dp, rows, slab), half_word),
            pltpu.VMEM((dp, rows, slab), half_word),
            pltpu.VMEM((dp, block, HEAD_DIM), half_word),
            pltpu.VMEM((dp * mp, block, HEAD_DIM), half_word),
            pltpu.VMEM((dp, block, HEAD_DIM), half_word),
            pltpu.VMEM((dp, block, HEAD_DIM), half_word),
            pltpu.VMEM((mp, block, HEAD_DIM), half_word),
            pltpu.VMEM((dp * mp, block, HEAD_DIM), half_word),
            pltpu.VMEM((mp, 1, HEAD_DIM), jnp.float32),
            pltpu.VMEM((dp * mp, 1, HEAD_DIM), jnp.float32),
            pltpu.VMEM((block, HEAD_DIM), half_word),
            pltpu.VMEM((mp, block, HEAD_DIM), half_word),
            pltpu.VMEM((dp, rows, out_slab), half_word),
            pltpu.VMEM((dp * mp, rows, out_slab), half_word),
            pltpu.SemaphoreType.DMA((11,)),
            pltpu.SemaphoreType.DMA((7,)),
            pltpu.SemaphoreType.DMA((7,)),
        ],
        compiler_params=pltpu.CompilerParams(collective_id=0, has_side_effects=True),
    )(
        lengths,
        windowed,
        hidden,
        in_gain,
        post_gain,
        query_weight,
        key_weight,
        value_weight,
        jnp.swapaxes(out_weight, 1, 2),
        key_cache.reshape(flat),
        value_cache.reshape(flat),
    )
    plain = pl.pallas_call(copy_kernel, out_shape=out_shape, in_specs=[vmem] * 3, out_specs=(vmem,) * 3)
    return plain(*(pltpu.with_memory_space_constraint(held, pltpu.VMEM) for held in results))


def device_step(hidden, *rest):
    fused = fits(hidden.shape[0], lax.axis_size("dp"), lax.axis_size("mp"))
    return (fused_device if fused else on_device)(hidden, *rest)


def solution(mesh):
    return jax.shard_map(
        device_step,
        mesh=mesh,
        in_specs=(
            P("dp", None),
            P(),
            P(),
            P(None, "dp", "mp"),
            P(None, "dp", "mp"),
            P(None, "dp", "mp"),
            P(None, "mp", "dp"),
            P(None, "dp", "mp", None, None),
            P(None, "dp", "mp", None, None),
            P("dp"),
            P(None, "dp"),
        ),
        out_specs=(P("dp", None), P(None, "dp", None, None), P(None, "dp", None, None)),
        check_vma=False,
    )
```

```python
import functools
import math

import jax
import jax.numpy as jnp
from jax import lax
from jax.experimental import pallas as pl
from jax.experimental.pallas import tpu as pltpu
from jax.sharding import PartitionSpec as P

HEADS = 16
KV_HEADS = 8
HEAD_DIM = 128
LAYERS = 1


EPSILON = 1e-06
SOFTCAP = 50.0
ROPE_BASE = 10000.0
NEGATIVE = -1e30


def rms_scale(values, gain_row):
    values = values.astype(jnp.float32)
    mean_square = jnp.mean(values * values, axis=-1, keepdims=True)
    return values * lax.rsqrt(mean_square + EPSILON) * gain_row.astype(jnp.float32)


def rotate(values, positions):
    half_dim = values.shape[-1] // 2
    frequency = jnp.power(
        ROPE_BASE, -2.0 * jnp.arange(half_dim, dtype=jnp.float32) / values.shape[-1]
    )
    angles = positions.astype(jnp.float32)[:, None] * frequency[None, :]
    cosine = jnp.cos(angles)[:, None, :]
    sine_table = jnp.sin(angles)[:, None, :]
    front_half = values[..., :half_dim]
    back_half = values[..., half_dim:]
    return jnp.concatenate(
        (
            front_half * cosine - back_half * sine_table,
            back_half * cosine + front_half * sine_table,
        ),
        axis=-1,
    )


def on_device(
    hidden,
    in_gain,
    post_gain,
    query_weight,
    key_weight,
    value_weight,
    out_weight,
    key_cache,
    value_cache,
    lengths,
    windowed,
):
    row_count = hidden.shape[0]
    query_width = query_weight.shape[2]
    key_width = key_weight.shape[2]
    seq_block = key_cache.shape[2]
    head_width = out_weight.shape[1]
    group_size = HEADS // KV_HEADS
    window_len = seq_block * lax.axis_size("mp") // 2
    keys_out = []
    values_out = []
    for layer_index in range(LAYERS):
        normed = rms_scale(hidden, in_gain[layer_index]).astype(jnp.bfloat16)
        token_slab = lax.all_to_all(normed, "dp", split_axis=1, concat_axis=0, tiled=True)
        joined = jnp.concatenate(
            (query_weight[layer_index], key_weight[layer_index], value_weight[layer_index]), 1
        )

        def local_term():
            part_rows = lax.slice_in_dim(token_slab, 0, row_count * lax.axis_size("dp"), axis=0)
            return jnp.dot(part_rows, joined, preferred_element_type=jnp.float32)

        summed = lax.psum_scatter(local_term(), "dp", scatter_dimension=0, tiled=True)
        query_part = summed[:, :query_width]
        key_part = summed[:, query_width : query_width + key_width]
        value_part = summed[:, query_width + key_width :]
        rounded = (
            query_part.astype(jnp.bfloat16),
            key_part.astype(jnp.bfloat16),
            value_part.astype(jnp.bfloat16),
        )
        query, key_raw, value_new = (
            lax.all_gather(rounded[0], "mp", axis=1, tiled=True),
            lax.all_gather(rounded[1], "mp", axis=1, tiled=True),
            lax.all_gather(rounded[2], "mp", axis=1, tiled=True),
        )
        queries = rotate(query.astype(jnp.float32).reshape(row_count, HEADS, HEAD_DIM), lengths)
        queries = (queries * HEAD_DIM ** (-0.5)).astype(jnp.bfloat16)
        keys_new = rotate(
            key_raw.astype(jnp.float32).reshape(row_count, KV_HEADS, HEAD_DIM), lengths
        ).astype(jnp.bfloat16)
        value_new = value_new.reshape(row_count, KV_HEADS, HEAD_DIM)
        grouped = queries.reshape(row_count, KV_HEADS, group_size, HEAD_DIM)
        scores = jnp.einsum(
            "rkgd,rskd->rkgs", grouped, key_cache[layer_index], preferred_element_type=jnp.float32
        )
        scores = SOFTCAP * jnp.tanh(scores / SOFTCAP)
        positions = lax.axis_index("mp") * seq_block + jnp.arange(seq_block, dtype=jnp.int32)
        window_flag = windowed[layer_index][:, None]
        usable = (positions[None, :] < lengths[:, None]) & (
            (window_flag == 0) | (positions[None, :] > lengths[:, None] - window_len)
        )
        usable = usable[:, None, None, :]
        masked = jnp.where(usable, scores, NEGATIVE)
        peaks = jnp.max(masked, axis=-1)
        exp_scores = jnp.where(usable, jnp.exp(masked - peaks[..., None]), 0.0)
        sums_exp = jnp.sum(exp_scores, axis=-1)
        accumulated = jnp.einsum(
            "rkgs,rskd->rkgd",
            exp_scores,
            value_cache[layer_index].astype(jnp.float32),
            preferred_element_type=jnp.float32,
        )
        global_peak = lax.pmax(peaks, "mp")
        rescale = jnp.exp(peaks - global_peak)
        sums_exp, accumulated = lax.psum(
            (sums_exp * rescale, accumulated * rescale[..., None]), "mp"
        )
        peaks = global_peak
        self_score = jnp.einsum(
            "rkgd,rkd->rkg", grouped, keys_new, preferred_element_type=jnp.float32
        )
        self_score = SOFTCAP * jnp.tanh(self_score / SOFTCAP)
        peak_all = jnp.maximum(peaks, self_score)
        old_scale = jnp.exp(peaks - peak_all)
        self_weight = jnp.exp(self_score - peak_all)
        denominator = sums_exp * old_scale + self_weight
        mixed = (
            accumulated * old_scale[..., None]
            + self_weight[..., None] * value_new.astype(jnp.float32)[:, :, None, :]
        )
        attended = (
            (mixed / denominator[..., None])
            .reshape(row_count, HEADS * HEAD_DIM)
            .astype(jnp.bfloat16)
        )
        attended_local = lax.dynamic_slice_in_dim(
            attended, lax.axis_index("mp") * head_width, head_width, 1
        )
        all_rows = lax.all_gather(attended_local, "dp", axis=0, tiled=True)
        partial_cols = jnp.dot(
            all_rows, out_weight[layer_index], preferred_element_type=jnp.float32
        )
        partial_cols = lax.psum(partial_cols, "mp")
        projected = lax.all_to_all(partial_cols, "dp", split_axis=0, concat_axis=1, tiled=True)
        hidden = (hidden.astype(jnp.float32) + rms_scale(projected, post_gain[layer_index])).astype(
            jnp.bfloat16
        )
        keys_out.append(keys_new)
        values_out.append(value_new)
    return (hidden, jnp.stack(keys_out), jnp.stack(values_out))


MESH_ID = pl.DeviceIdType.MESH
TILE_ROWS = 8


def fits(rows, dp, mp):
    return (
        mp & (mp - 1) == 0
        and dp & (dp - 1) == 0
        and HEADS % mp == 0
        and KV_HEADS % mp == 0
        and HEADS == 2 * KV_HEADS
        and rows * HEADS // mp == TILE_ROWS
    )


def low(index, size):
    return index & (size - 1)


def high(index, size):
    return index >> (size.bit_length() - 1)


def one_hot(rows, columns, match):
    row = lax.broadcasted_iota(jnp.int32, (rows, columns), 0)
    column = lax.broadcasted_iota(jnp.int32, (rows, columns), 1)
    return jnp.where(match(row, column), 1.0, 0.0).astype(jnp.bfloat16)


def partners(mine, count):
    found = []
    for pattern in range(count):
        there = 0
        for bit in range(count.bit_length() - 1):
            held = lax.rem(mine // 2**bit, 2)
            there = there + 2**bit * (1 - held if pattern >> bit & 1 else held)
        found.append(there)
    return found


def pick(selector, values):
    return jnp.dot(selector, values, preferred_element_type=jnp.float32)


def fused_kernel(
    dp,
    mp,
    lengths_hbm,
    windowed_hbm,
    hidden_hbm,
    in_gain_hbm,
    post_gain_hbm,
    query_hbm,
    key_hbm,
    value_hbm,
    out_hbm,
    key_cache_hbm,
    value_cache_hbm,
    hidden_out_ref,
    new_keys_ref,
    new_values_ref,
    lengths_ref,
    windowed_ref,
    hidden_ref,
    in_gain_ref,
    post_gain_ref,
    query_w,
    key_w,
    value_w,
    out_w,
    keys,
    values,
    norm_send,
    norm_recv,
    query_send,
    query_recv,
    pair_send,
    pair_recv,
    mix_send,
    mix_recv,
    sums_send,
    sums_recv,
    token_send,
    token_recv,
    cols_send,
    cols_recv,
    load_sem,
    send_sem,
    recv_sem,
):
    my_dp = lax.axis_index("dp")
    my_mp = lax.axis_index("mp")
    devices = dp * mp
    me = my_dp * mp + my_mp
    rows = hidden_ref.shape[0]
    total_rows = rows * dp
    slab = norm_send.shape[2]
    query_width = query_w.shape[1]
    key_width = key_w.shape[1]
    query_heads = query_width // HEAD_DIM
    key_heads = key_width // HEAD_DIM
    cache_rows = key_cache_hbm.shape[2]
    seq_block = cache_rows // KV_HEADS
    window_len = seq_block * mp // 2

    loads = [
        pltpu.make_async_copy(src, dst, load_sem.at[i])
        for i, (src, dst) in enumerate(
            (
                (hidden_hbm, hidden_ref),
                (in_gain_hbm, in_gain_ref),
                (lengths_hbm, lengths_ref),
                (windowed_hbm, windowed_ref),
                (query_hbm.at[0], query_w),
                (key_hbm.at[0], key_w),
                (value_hbm.at[0], value_w),
                (key_cache_hbm.at[0], keys),
                (value_cache_hbm.at[0], values),
                (out_hbm.at[0], out_w),
                (post_gain_hbm, post_gain_ref),
            )
        )
    ]
    peer_dp = partners(my_dp, dp)
    peer_mp = partners(my_mp, mp)
    others = [(i, j) for i in reversed(range(dp)) for j in reversed(range(mp)) if i + j > 0]
    barrier = pltpu.get_barrier_semaphore()
    for i, j in others:
        pl.semaphore_signal(
            barrier,
            inc=1,
            device_id={"dp": peer_dp[i], "mp": peer_mp[j]},
            device_id_type=MESH_ID,
        )
    for load in loads:
        load.start()
    for load in loads[:2]:
        load.wait()

    hidden = hidden_ref[...].astype(jnp.float32)
    mean_square = jnp.mean(hidden * hidden, axis=-1, keepdims=True)
    normed = hidden * lax.rsqrt(mean_square + EPSILON) * in_gain_ref[...]
    for part in range(dp):
        norm_send[part] = normed[:, part * slab : (part + 1) * slab].astype(jnp.bfloat16)

    pl.semaphore_wait(barrier, devices - 1)
    def finish(buffer, count, sem):
        block = buffer.at[pl.ds(0, count)]
        pltpu.make_async_copy(block, block, sem).wait()

    def exchange(recv, stage, targets, source, slot):
        for i, j in targets:
            pltpu.make_async_remote_copy(
                src_ref=source(peer_dp[i], peer_mp[j]),
                dst_ref=recv.at[slot],
                send_sem=send_sem.at[stage],
                recv_sem=recv_sem.at[stage],
                device_id={"dp": peer_dp[i], "mp": peer_mp[j]},
                device_id_type=MESH_ID,
            ).start()

    along_dp = [(i, j) for i, j in others if j == 0]
    along_mp = [(i, j) for i, j in others if i == 0]
    exchange(norm_recv, 0, along_dp, lambda a, b: norm_send.at[a], my_dp)
    norm_recv[my_dp] = norm_send[my_dp]
    for load in loads[2:4]:
        load.wait()

    block = rows * query_heads
    half = HEAD_DIM // 2
    lane = lax.broadcasted_iota(jnp.int32, (block, HEAD_DIM), 1)
    request = high(lax.broadcasted_iota(jnp.int32, (block, HEAD_DIM), 0), query_heads)
    pair = low(lane, half).astype(jnp.float32)
    frequency = jnp.exp(pair * (-2.0 / HEAD_DIM * math.log(ROPE_BASE)))
    place = jnp.full((block, HEAD_DIM), lengths_ref[0], jnp.int32)
    for r in range(1, rows):
        place = jnp.where(request == r, lengths_ref[r], place)
    angle = place.astype(jnp.float32) * frequency
    cosine = jnp.cos(angle)
    sine = jnp.sin(angle)
    sine = jnp.where(lane < half, -sine, sine)

    for load in loads[4:7]:
        load.wait()
    finish(norm_recv, dp - 1, recv_sem.at[0])
    tokens = jnp.concatenate(
        [norm_recv[part].astype(jnp.float32) for part in range(dp)], axis=0
    ).astype(jnp.bfloat16)
    spread = one_hot(
        total_rows * query_heads,
        total_rows * query_heads,
        lambda row, column: column
        == low(row, query_heads) * total_rows + high(row, query_heads),
    )

    def by_owner(parts):
        pieces = [
            part[:, at : at + HEAD_DIM]
            for part in parts
            for at in range(0, part.shape[1], HEAD_DIM)
        ]
        stacked = jnp.concatenate(pieces, axis=0).astype(jnp.bfloat16)
        return pick(spread, stacked).astype(jnp.bfloat16).reshape(dp, block, HEAD_DIM)

    query_send[...] = by_owner([pick(tokens, query_w[...])])
    exchange(query_recv, 1, others, lambda a, b: query_send.at[a], me)
    query_recv[me] = query_send[my_dp]
    pair_send[...] = by_owner([pick(tokens, key_w[...]), pick(tokens, value_w[...])])
    exchange(pair_recv, 2, along_dp, lambda a, b: pair_send.at[a], my_dp)
    pair_recv[my_dp] = pair_send[my_dp]

    for load in loads[7:9]:
        load.wait()
    group_rows = mp * block
    row = lax.broadcasted_iota(jnp.int32, (group_rows, cache_rows), 0)
    column = lax.broadcasted_iota(jnp.int32, (group_rows, cache_rows), 1)
    head_match = low(column, KV_HEADS) == high(row, block) * key_heads + high(
        low(row, query_heads), 2
    )
    row_request = high(low(row, block), query_heads)
    position = my_mp * seq_block + high(column, KV_HEADS)
    allowed = []
    for r in range(rows):
        length = lengths_ref[r]
        floor = jnp.where(windowed_ref[0, r] == 0, -1, length - window_len)
        allowed.append(
            head_match & (row_request == r) & (position < length) & (position > floor)
        )
    own_row = lax.broadcasted_iota(jnp.int32, (group_rows, block), 0)
    own_column = lax.broadcasted_iota(jnp.int32, (group_rows, block), 1)
    own_base = low(own_row, block) - low(own_row, query_heads) + high(low(own_row, query_heads), 2)
    own_group = high(own_row, block) == my_mp
    own_key = own_group & (own_column == own_base)
    own_value = jnp.where(own_column == own_base + key_heads, 1.0, 0.0).astype(jnp.bfloat16)
    group_lane = lax.broadcasted_iota(jnp.int32, (group_rows, HEAD_DIM), 1)
    group_row = low(lax.broadcasted_iota(jnp.int32, (group_rows, HEAD_DIM), 0), block)
    over_last = (((1,), (1,)), ((), ()))

    def turn(raw):
        return raw * cosine + pltpu.roll(raw, half, raw.ndim - 1) * sine

    finish(query_recv, devices - 1, recv_sem.at[1])
    raw = jnp.sum(
        query_recv[...].astype(jnp.float32).reshape(dp, mp, block, HEAD_DIM), axis=0
    )
    raw = raw.astype(jnp.bfloat16).astype(jnp.float32)
    queries = jnp.concatenate([turn(raw[m]) for m in range(mp)], axis=0)
    queries = (queries * HEAD_DIM ** (-0.5)).astype(jnp.bfloat16)
    accumulated = jnp.zeros((group_rows, HEAD_DIM), jnp.float32)
    sums_exp = jnp.zeros((group_rows, 1), jnp.float32)
    for r in range(rows):
        scores = lax.dot_general(
            queries, keys[r], over_last, preferred_element_type=jnp.float32
        )
        scores = SOFTCAP * jnp.tanh(scores * (1.0 / SOFTCAP))
        exp_scores = jnp.where(allowed[r], jnp.exp(scores), 0.0)
        sums_exp = sums_exp + jnp.sum(exp_scores, axis=-1, keepdims=True)
        accumulated = accumulated + pick(exp_scores.astype(jnp.bfloat16), values[r])

    finish(pair_recv, dp - 1, recv_sem.at[2])
    pair_raw = jnp.sum(pair_recv[...].astype(jnp.float32), axis=0).astype(jnp.bfloat16)
    pair_wide = pair_raw.astype(jnp.float32)
    token = turn(pair_wide).astype(jnp.bfloat16)
    own = lax.dot_general(queries, token, over_last, preferred_element_type=jnp.float32)
    own = jnp.sum(jnp.where(own_key, own, 0.0), axis=-1, keepdims=True)
    own = jnp.exp(SOFTCAP * jnp.tanh(own * (1.0 / SOFTCAP)))
    own = jnp.where(own_group[:, :1], own, 0.0)
    accumulated = accumulated + own * pick(own_value, pair_raw)
    sums_exp = sums_exp + own
    mix_send[...] = accumulated.reshape(mp, block, HEAD_DIM).astype(mix_send.dtype)
    sums_send[...] = jnp.sum(
        jnp.where(group_lane == group_row, sums_exp, 0.0).reshape(mp, block, HEAD_DIM),
        axis=1,
        keepdims=True,
    )
    exchange(mix_recv, 3, others, lambda a, b: mix_send.at[b], me)
    exchange(sums_recv, 4, others, lambda a, b: sums_send.at[b], me)
    mix_recv[me] = mix_send[my_mp]
    sums_recv[me] = sums_send[my_mp]
    is_key = low(lax.broadcasted_iota(jnp.int32, (block, HEAD_DIM), 0), query_heads) < key_heads
    token_send[...] = jnp.where(is_key, token.astype(jnp.float32), pair_wide).astype(jnp.bfloat16)
    exchange(token_recv, 5, along_mp, lambda a, b: token_send, my_mp)
    token_recv[my_mp] = token_send[...]

    for load in loads[9:]:
        load.wait()
    finish(mix_recv, devices - 1, recv_sem.at[3])
    mixed = jnp.sum(
        mix_recv[...].astype(jnp.float32).reshape(dp, mp, block, HEAD_DIM), axis=1
    )
    finish(sums_recv, devices - 1, recv_sem.at[4])
    sums = jnp.sum(sums_recv[...].reshape(dp, mp, 1, HEAD_DIM), axis=1)
    at_row = lax.broadcasted_iota(jnp.int32, mixed.shape, 1)
    at_lane = lax.broadcasted_iota(jnp.int32, mixed.shape, 2)
    sums = jnp.sum(jnp.where(at_row == at_lane, sums, 0.0), axis=-1, keepdims=True)
    attended = (mixed / sums).reshape(total_rows, query_heads, HEAD_DIM)
    heads = jnp.concatenate(
        [attended[:, b, :] for b in range(query_heads)], axis=1
    ).astype(jnp.bfloat16)
    partial_cols = lax.dot_general(
        heads, out_w[...], over_last, preferred_element_type=jnp.float32
    )
    for part in range(dp):
        cols_send[part] = partial_cols[part * rows : (part + 1) * rows].astype(cols_send.dtype)
    exchange(cols_recv, 6, others, lambda a, b: cols_send.at[a], me)
    cols_recv[me] = cols_send[my_dp]

    def owner(row, first):
        head = low(row, KV_HEADS)
        return (
            high(head, key_heads) * block
            + high(row, KV_HEADS) * query_heads
            + first
            + low(head, key_heads)
        )

    finish(token_recv, mp - 1, recv_sem.at[5])
    tokens_new = token_recv[...].astype(jnp.float32).reshape(group_rows, HEAD_DIM)
    tokens_new = tokens_new.astype(jnp.bfloat16)
    for first, out_ref in ((0, new_keys_ref), (key_heads, new_values_ref)):
        chosen = one_hot(
            rows * KV_HEADS, group_rows, lambda row, column: column == owner(row, first)
        )
        out_ref[...] = pick(chosen, tokens_new).astype(jnp.bfloat16).reshape(out_ref.shape)
    finish(cols_recv, devices - 1, recv_sem.at[6])
    pieces = []
    for part in range(dp):
        piece = cols_recv[part * mp].astype(jnp.float32)
        for other in range(1, mp):
            piece = piece + cols_recv[part * mp + other].astype(jnp.float32)
        pieces.append(piece)
    projected = jnp.concatenate(pieces, axis=1)
    mean_square = jnp.mean(projected * projected, axis=-1, keepdims=True)
    update = projected * lax.rsqrt(mean_square + EPSILON) * post_gain_ref[...]
    hidden_out_ref[...] = (hidden_ref[...].astype(jnp.float32) + update).astype(jnp.bfloat16)

    finish(norm_recv, dp - 1, send_sem.at[0])
    finish(query_recv, devices - 1, send_sem.at[1])
    finish(pair_recv, dp - 1, send_sem.at[2])
    finish(mix_recv, devices - 1, send_sem.at[3])
    finish(sums_recv, devices - 1, send_sem.at[4])
    finish(token_recv, mp - 1, send_sem.at[5])
    finish(cols_recv, devices - 1, send_sem.at[6])


def copy_kernel(a_ref, b_ref, c_ref, a_out, b_out, c_out):
    a_out[...] = a_ref[...]
    b_out[...] = b_ref[...]
    c_out[...] = c_ref[...]


def fused_device(
    hidden,
    in_gain,
    post_gain,
    query_weight,
    key_weight,
    value_weight,
    out_weight,
    key_cache,
    value_cache,
    lengths,
    windowed,
):
    dp = lax.axis_size("dp")
    mp = lax.axis_size("mp")
    rows = hidden.shape[0]
    slab = query_weight.shape[1]
    out_slab = out_weight.shape[2]
    block = rows * query_weight.shape[2] // HEAD_DIM
    half_word = jnp.bfloat16
    flat = (LAYERS, rows, key_cache.shape[2] * KV_HEADS, HEAD_DIM)
    out_shape = (
        jax.ShapeDtypeStruct(hidden.shape, half_word),
        jax.ShapeDtypeStruct((LAYERS, rows, KV_HEADS, HEAD_DIM), half_word),
        jax.ShapeDtypeStruct((LAYERS, rows, KV_HEADS, HEAD_DIM), half_word),
    )
    vmem = pl.BlockSpec(memory_space=pltpu.VMEM)
    far = pl.BlockSpec(memory_space=pl.ANY)
    results = pl.pallas_call(
        functools.partial(fused_kernel, dp, mp),
        out_shape=tuple(pltpu.VMEM(held.shape, held.dtype) for held in out_shape),
        in_specs=[far] * 11,
        out_specs=(vmem, vmem, vmem),
        scratch_shapes=[
            pltpu.SMEM(lengths.shape, lengths.dtype),
            pltpu.SMEM(windowed.shape, windowed.dtype),
            pltpu.VMEM(hidden.shape, hidden.dtype),
            pltpu.VMEM(in_gain.shape, in_gain.dtype),
            pltpu.VMEM(post_gain.shape, post_gain.dtype),
            pltpu.VMEM(query_weight.shape[1:], half_word),
            pltpu.VMEM(key_weight.shape[1:], half_word),
            pltpu.VMEM(value_weight.shape[1:], half_word),
            pltpu.VMEM((out_slab, out_weight.shape[1]), half_word),
            pltpu.VMEM(flat[1:], half_word),
            pltpu.VMEM(flat[1:], half_word),
            pltpu.VMEM((dp, rows, slab), half_word),
            pltpu.VMEM((dp, rows, slab), half_word),
            pltpu.VMEM((dp, block, HEAD_DIM), half_word),
            pltpu.VMEM((dp * mp, block, HEAD_DIM), half_word),
            pltpu.VMEM((dp, block, HEAD_DIM), half_word),
            pltpu.VMEM((dp, block, HEAD_DIM), half_word),
            pltpu.VMEM((mp, block, HEAD_DIM), half_word),
            pltpu.VMEM((dp * mp, block, HEAD_DIM), half_word),
            pltpu.VMEM((mp, 1, HEAD_DIM), jnp.float32),
            pltpu.VMEM((dp * mp, 1, HEAD_DIM), jnp.float32),
            pltpu.VMEM((block, HEAD_DIM), half_word),
            pltpu.VMEM((mp, block, HEAD_DIM), half_word),
            pltpu.VMEM((dp, rows, out_slab), half_word),
            pltpu.VMEM((dp * mp, rows, out_slab), half_word),
            pltpu.SemaphoreType.DMA((11,)),
            pltpu.SemaphoreType.DMA((7,)),
            pltpu.SemaphoreType.DMA((7,)),
        ],
        compiler_params=pltpu.CompilerParams(collective_id=0, has_side_effects=True),
    )(
        lengths,
        windowed,
        hidden,
        in_gain,
        post_gain,
        query_weight,
        key_weight,
        value_weight,
        jnp.swapaxes(out_weight, 1, 2),
        key_cache.reshape(flat),
        value_cache.reshape(flat),
    )
    plain = pl.pallas_call(copy_kernel, out_shape=out_shape, in_specs=[vmem] * 3, out_specs=(vmem,) * 3)
    return plain(*(pltpu.with_memory_space_constraint(held, pltpu.VMEM) for held in results))


def device_step(hidden, *rest):
    fused = fits(hidden.shape[0], lax.axis_size("dp"), lax.axis_size("mp"))
    return (fused_device if fused else on_device)(hidden, *rest)


def solution(mesh):
    return jax.shard_map(
        device_step,
        mesh=mesh,
        in_specs=(
            P("dp", None),
            P(),
            P(),
            P(None, "dp", "mp"),
            P(None, "dp", "mp"),
            P(None, "dp", "mp"),
            P(None, "mp", "dp"),
            P(None, "dp", "mp", None, None),
            P(None, "dp", "mp", None, None),
            P("dp"),
            P(None, "dp"),
        ),
        out_specs=(P("dp", None), P(None, "dp", None, None), P(None, "dp", None, None)),
        check_vma=False,
    )
```
